256 devices in a mesh: lon: 16 (over z, y_hi), lat: 8 (over x, core), mem: 2 (over y_lo).
Axes of the slice: x: 4, y: 4 (y_hi: 2, y_lo: 2; y = y_hi * 2 + y_lo), z: 8, core: 2. Of those that a mesh axis runs over, the one named last changes fastest.
Arguments:
- tokens: bfloat16 [4, 8, 272, 96, 192], P('mem', None, 'lat', 'lon'), parts along dimension 0, may hold values from -6 to 6
- band_rows: int32 [8, 2], P('lat'), may hold values from 0 to 177, as said below
- down_gain: float32 [768], replicated, may hold values from 0.1 to 1.9
- down_shift: float32 [768], replicated, may hold values from -3 to 3
- down_weight: bfloat16 [768, 384], P(('lon', 'lat')), may hold values from -0.21875 to 0.21875
- up_weight: bfloat16 [384, 768], P(('lon', 'lat')), may hold values from -0.3125 to 0.3125
- up_gain: float32 [192], replicated, may hold values from 0.1 to 1.9
- up_shift: float32 [192], replicated, may hold values from -3 to 3
- mix_weight: bfloat16 [192, 192], replicated, may hold values from -0.4375 to 0.4375
Outputs:
- expanded: bfloat16 [4, 8, 272, 96, 192], P('mem', None, 'lat', 'lon'), parts along dimension 0
The draws below stay inside these ranges and needn't reach their ends.
There are 2 independent parts, one for each index of `mem`. The reference program is written for one: setup_inputs(seed, part) draws one part's arguments, and reference() takes and returns one part's arrays. A program takes and returns all parts, laid end to end along the dimension named above; an argument that names none is the same for every part. Nothing has to cross between parts.
Inputs may be any that keep to these rules, and one draw needn't show every extreme that they name: `band_rows`: row b holds band b's first latitude row and one past its last; the bands cover rows 0 to 176 in order without gaps; band 0 holds an odd number of rows and every other band an even number; each band holds at least 2 * (5) rows and at most 34, and some band other than band 0 holds exactly 34.
All inputs are finite; a program needn't handle non-finite values.
Results may differ from the reference program's by a relative error of at most 0.0062.
Values may be sent and summed in bfloat16 or wider, within the bound.
A program may use at most 64 MiB of HBM per device.

```python
import jax
import jax.numpy as jnp
from jax import lax

C = 192
LEVELS = 8
MEMBERS = 2
BAND_ROWS = 22
BAND_ROW_SLOTS = 34
SLOTS = 272
LAT = 177
LON = 96
N_LAT = 8


def draw_band_rows(key, part):
    bands = N_LAT
    half_least = BAND_ROWS // 4
    slot_half = BAND_ROW_SLOTS // 2
    band_ids = jnp.arange(bands, dtype=jnp.int32)
    fullest = jax.random.randint(jax.random.fold_in(key, 11), (), 1, bands, dtype=jnp.int32)
    weights = jax.random.randint(jax.random.fold_in(key, 12), (bands,), 500, 1001, dtype=jnp.int32)
    order_keys = jax.random.permutation(jax.random.fold_in(key, 13), bands).astype(jnp.int32)
    sharing = band_ids != fullest
    weights = jnp.where(sharing, weights, 0)
    spare_halves = BAND_ROWS * bands // 2 - slot_half - (bands - 1) * half_least
    half_shares = spare_halves * weights // jnp.sum(weights)
    leftover = spare_halves - jnp.sum(half_shares)
    earlier = sharing[None, :] & (order_keys[None, :] < order_keys[:, None])
    ranking = jnp.sum(earlier.astype(jnp.int32), axis=1)
    extra_halves = (sharing & (ranking < leftover)).astype(jnp.int32)
    halves = jnp.where(band_ids == fullest, slot_half, half_least + half_shares + extra_halves)
    row_counts = (2 * halves + (band_ids == 0).astype(jnp.int32)).astype(jnp.int32)
    starts = jnp.cumsum(row_counts) - row_counts
    return jnp.stack([starts, starts + row_counts], axis=1).astype(jnp.int32)


def level_of(stream_key, extent, shards, smallest, top_value):
    def one(axis_at, parts):
        heights = jax.random.uniform(jax.random.fold_in(jax.random.fold_in(stream_key, 6), axis_at), (parts,), jnp.float32, smallest / len(shards), top_value / len(shards))
        return jnp.repeat(jnp.exp(heights), extent[axis_at] // parts).reshape((-1,) + (1,) * (len(extent) - axis_at - 1))

    level = one(*shards[0])
    for cut in shards[1:]:
        level = level * one(*cut)
    return level


def scatter_about(rng, dims, scale, most, cuts=(), kind=jnp.bfloat16):
    values = scale * jax.random.normal(rng, dims, jnp.float32)
    if cuts:
        values = values * level_of(rng, dims, cuts, -0.22, 0.18)
    return jnp.clip(values, -most, most).astype(kind)


def setup_inputs(seed: int = 0, part: int = 0) -> dict:
    streams_of = jax.random.split(jax.random.key(seed), 10)
    part_keys = jax.random.split(jax.random.fold_in(streams_of[9], part), 10)
    return {
        "tokens": scatter_about(part_keys[0], (MEMBERS, LEVELS, SLOTS, LON, C), 1.0, 6.0, ((2, 8), (3, 16))),
        "band_rows": draw_band_rows(jax.random.fold_in(streams_of[9], 71), part),
        "down_gain": jnp.clip(1.0 + 0.18 * jax.random.normal(streams_of[2], (4 * C,), jnp.float32), 0.1, 1.9),
        "down_shift": scatter_about(streams_of[3], (4 * C,), 0.5, 3.0, (), jnp.float32),
        "down_weight": scatter_about(streams_of[4], (4 * C, 2 * C), (4 * C) ** -0.5, 0.21875, ((0, 128),)),
        "up_weight": scatter_about(streams_of[5], (2 * C, 4 * C), (2 * C) ** -0.5, 0.3125, ((0, 128),)),
        "up_gain": jnp.clip(1.0 + 0.18 * jax.random.normal(streams_of[6], (C,), jnp.float32), 0.1, 1.9),
        "up_shift": scatter_about(streams_of[7], (C,), 0.5, 3.0, (), jnp.float32),
        "mix_weight": scatter_about(streams_of[8], (C, C), C ** -0.5, 0.4375),
    }


def normalize(values, scale_gain, bias_shift):
    average = lax.optimization_barrier(jnp.mean(values, axis=-1, keepdims=True))
    centred = values - average
    spread = lax.optimization_barrier(jnp.mean(centred * centred, axis=-1, keepdims=True))
    return centred * lax.rsqrt(spread + 1e-05) * scale_gain + bias_shift

def reference(tokens, band_rows, down_gain, down_shift, down_weight, up_weight, up_gain, up_shift, mix_weight):
    band_starts = band_rows[:, 0].astype(jnp.int32)
    band_ends = band_rows[:, 1].astype(jnp.int32)
    lat_rows = jnp.arange(LAT, dtype=jnp.int32)
    band_of = (lax.optimization_barrier(jnp.sum((lat_rows[:, None] >= band_starts[None, :]).astype(jnp.int32), axis=1)) - 1).astype(jnp.int32)
    source = (band_of * BAND_ROW_SLOTS + lat_rows - jnp.take(band_starts, band_of)).astype(jnp.int32)
    half_lat = (LAT + 1) // 2
    half_lon = LON // 2
    slot_ids = jnp.arange(SLOTS, dtype=jnp.int32)
    slot_band = (slot_ids // BAND_ROW_SLOTS).astype(jnp.int32)
    local_row = (slot_ids % BAND_ROW_SLOTS).astype(jnp.int32)
    live_rows = jnp.take(band_ends, slot_band) - jnp.take(band_starts, slot_band)
    global_row = (jnp.take(band_starts, slot_band) + local_row).astype(jnp.int32)
    is_live = local_row < live_rows
    safe_row = jnp.minimum(global_row, LAT - 1).astype(jnp.int32)

    def one_level(level_plane):
        field = jnp.take(level_plane, source, axis=0)
        field = jnp.pad(field, ((0, 1), (0, 0), (0, 0)))
        field = jnp.roll(field, -1, axis=1)
        blocks = field.reshape(half_lat, 2, half_lon, 2, C).transpose(0, 2, 3, 1, 4).reshape(half_lat * half_lon, 4 * C)
        merged_norm = normalize(blocks.astype(jnp.float32), down_gain, down_shift).astype(jnp.bfloat16)
        coarse = jnp.dot(merged_norm, down_weight, preferred_element_type=jnp.float32).astype(jnp.bfloat16)
        grown = jnp.dot(coarse, up_weight, preferred_element_type=jnp.float32)
        grown = grown.reshape(half_lat, half_lon, 2, 2, C).transpose(0, 2, 1, 3, 4).reshape(2 * half_lat, 2 * half_lon, C)[:LAT]
        grown = jnp.roll(grown, 1, axis=1)
        fine_norm = normalize(grown, up_gain, up_shift).astype(jnp.bfloat16)
        fine_out = jnp.dot(fine_norm.reshape(LAT * LON, C), mix_weight, preferred_element_type=jnp.float32)
        fine_out = fine_out.astype(jnp.bfloat16).reshape(LAT, LON, C)
        picked = jnp.take(fine_out, safe_row, axis=0)
        return jnp.where(is_live[:, None, None], picked, jnp.zeros_like(picked))
    planes = tokens.reshape(MEMBERS * LEVELS, SLOTS, LON, C)
    results = lax.map(one_level, planes)
    return results.reshape(MEMBERS, LEVELS, SLOTS, LON, C)
```

```python
import functools

import jax
import jax.numpy as jnp
from jax import lax
from jax.experimental import pallas as pl
from jax.experimental.pallas import tpu as pltpu
from jax.sharding import PartitionSpec as P

MESH = pl.DeviceIdType.MESH
MEMBERS, LEVELS, SLOTS, COLS, C = 2, 8, 34, 6, 192
EXT = SLOTS + 2
HALF = EXT // 2
NZ = 8
PIECES = 3
BF = jnp.bfloat16
F32 = jnp.float32


def exchange(
    band_ref, tok_hbm, down_hbm, up_hbm,
    wd, wu, west, east, north, south,
    tok, last, own_d, own_u, got_d, got_u, flat_d, flat_u,
    load_sem, s1_send, s1_recv, ring_send, ring_recv, pair_send, pair_recv,
    col_send, col_recv, row_send, row_recv,
):
    lon, lat, mem = lax.axis_index("lon"), lax.axis_index("lat"), lax.axis_index("mem")
    z, yh = lon // 2, lon % 2
    core, xx = lat % 2, lat // 2

    def at(lon_, lat_, mem_):
        return (lon_, lat_, mem_)

    def other(yh_):
        return 2 * z + yh_

    loads = [
        pltpu.make_async_copy(down_hbm, own_d, load_sem.at[0]),
        pltpu.make_async_copy(up_hbm, own_u, load_sem.at[1]),
        pltpu.make_async_copy(tok_hbm, tok, load_sem.at[2]),
    ]
    for load in loads:
        load.start()

    lon_w, lon_e = (lon + 15) % 16, (lon + 1) % 16
    lat_n, lat_s = (lat + 7) % 8, (lat + 1) % 8
    up_z = ((z + 1) % NZ) * 2 + yh
    dn_z = ((z + NZ - 1) % NZ) * 2 + yh
    barrier = pltpu.get_barrier_semaphore()

    def greet(where):
        pl.semaphore_signal(barrier, inc=1, device_id=where, device_id_type=MESH)

    for d in range(1, 8):
        greet(at(lon, (lat + d) % 8, mem))
    for d in range(8):
        greet(at(other(1 - yh), (lat + d) % 8, 1 - mem))
    for where in (
        at(up_z, lat, mem), at(dn_z, lat, mem), at(lon_w, lat, mem), at(lon_e, lat, mem),
        at(lon_w, lat_n, mem), at(lon_w, lat_s, mem), at(lon_e, lat_n, mem), at(lon_e, lat_s, mem),
    ):
        greet(where)
    loads[0].wait()
    loads[1].wait()
    pl.semaphore_wait(barrier, 23)

    me = yh * 8 + lat

    def copy(src, dst, ssem, rsem, where):
        return pltpu.make_async_remote_copy(
            src_ref=src, dst_ref=dst, send_sem=ssem, recv_sem=rsem,
            device_id=where, device_id_type=MESH,
        )

    def stage_one(src, got, kind, base):
        out = []
        for d in range(4):
            lat_t = 2 * ((xx + d) % 4) + kind
            out.append((d, 0, copy(src, got.at[me], s1_send.at[base + d], s1_recv.at[me], at(lon, lat_t, mem))))
            out.append((d, 1, copy(src, got.at[me], s1_send.at[base + 4 + d], s1_recv.at[me], at(other(1 - yh), lat_t, 1 - mem))))
        return out

    sends = [(0, s) for s in stage_one(own_d, got_d, 0, 0)] + [(1, s) for s in stage_one(own_u, got_u, 1, 8)]
    for kind, (d, far, cp) in sends:
        if d == 0 and far == 0:
            @pl.when(core != kind)
            def _():
                cp.start()
        else:
            cp.start()

    loads[2].wait()
    cols = [
        copy(tok.at[:, :, 0], east, col_send.at[0], col_recv.at[0], at(lon_w, lat, mem)),
        copy(tok.at[:, :, COLS - 1], west, col_send.at[1], col_recv.at[1], at(lon_e, lat, mem)),
    ]
    for cp in cols:
        cp.start()

    live = band_ref[0, 1] - band_ref[0, 0]
    last[...] = tok[:, pl.ds(jnp.clip(live - 1, 0, SLOTS - 1), 1)].reshape(MEMBERS, COLS, LEVELS, C)
    to_next = [
        copy(last, north.at[:, 1 : COLS + 1], row_send.at[0], row_recv.at[0], at(lon, lat_s, mem)),
        copy(last.at[:, 0], north.at[:, COLS + 1], row_send.at[1], row_recv.at[1], at(lon_w, lat_s, mem)),
        copy(last.at[:, COLS - 1], north.at[:, 0], row_send.at[2], row_recv.at[2], at(lon_e, lat_s, mem)),
    ]
    to_prev = [
        copy(tok.at[:, 0], south.at[:, 1 : COLS + 1], row_send.at[3], row_recv.at[3], at(lon, lat_n, mem)),
        copy(tok.at[:, 0, 0], south.at[:, COLS + 1], row_send.at[4], row_recv.at[4], at(lon_w, lat_n, mem)),
        copy(tok.at[:, 0, COLS - 1], south.at[:, 0], row_send.at[5], row_recv.at[5], at(lon_e, lat_n, mem)),
    ]

    @pl.when(lat < 7)
    def _():
        for cp in to_next:
            cp.start()

    @pl.when(lat > 0)
    def _():
        for cp in to_prev:
            cp.start()

    @pl.when(lat == 7)
    def _():
        south[...] = jnp.zeros_like(south)

    @pl.when(lat == 0)
    def _():
        north[...] = jnp.zeros_like(north)

    def gather(kind, own, got, flat, full, rows):
        part = 16 * rows // PIECES
        got[pl.ds(me, 1)] = own[...].reshape(1, *own.shape)
        for d in range(1, 16):
            i = (me + d) % 16
            copy(own, got.at[i], s1_send.at[0], s1_recv.at[i], at(lon, lat, mem)).wait_recv()
        for i in range(16):
            flat[rows * i : rows * (i + 1), :] = got[i].astype(F32)
        full[pl.ds(z, 1)] = flat[...].astype(BF).reshape(1, *flat.shape)

        def block(step, way):
            return (z + NZ + (step if way else -step)) % NZ

        def piece(b, k):
            return full.at[b, part * k : part * (k + 1)]

        def ring(step, way, k):
            b = block(step, way)
            return copy(
                piece(b, k), piece(b, k), ring_send.at[way, step, k], ring_recv.at[way, step, k],
                at(dn_z if way else up_z, lat, mem),
            )

        def landed(step, way, k):
            b = block(step + 1, way)
            return copy(
                piece(b, k), piece(b, k), ring_send.at[way, step, k], ring_recv.at[way, step, k],
                at(dn_z if way else up_z, lat, mem),
            )

        def pair(b):
            return copy(full.at[b], full.at[b], pair_send.at[b], pair_recv.at[b], at(lon, lat + 1 - 2 * core, mem))

        steps = (4, 3)
        for k in range(PIECES):
            for way in range(2):
                ring(0, way, k).start()
        pair(z).start()
        for step in range(4):
            for k in range(PIECES):
                for way in range(2):
                    if step < steps[way]:
                        landed(step, way, k).wait_recv()
                        if step + 1 < steps[way]:
                            ring(step + 1, way, k).start()
            for way in range(2):
                if step < steps[way]:
                    pair(block(step + 1, way)).start()
        for step in range(4):
            for k in range(PIECES):
                for way in range(2):
                    if step < steps[way]:
                        ring(step, way, k).wait_send()
        for b in range(NZ):
            pair(b).wait_send()

    def take(full):
        for b in range(NZ):
            copy(full.at[b], full.at[b], pair_send.at[b], pair_recv.at[b], at(lon, lat, mem)).wait_recv()

    @pl.when(core == 0)
    def _():
        gather(0, own_d, got_d, flat_d, wd, 6)
        take(wu)

    @pl.when(core == 1)
    def _():
        gather(1, own_u, got_u, flat_u, wu, 3)
        take(wd)

    for kind, (d, far, cp) in sends:
        if d == 0 and far == 0:
            @pl.when(core != kind)
            def _():
                cp.wait_send()
        else:
            cp.wait_send()
    for cp in cols:
        cp.wait()

    @pl.when(lat < 7)
    def _():
        for cp in to_next:
            cp.wait_send()
        for cp in to_prev:
            cp.wait_recv()

    @pl.when(lat > 0)
    def _():
        for cp in to_prev:
            cp.wait_send()
        for cp in to_next:
            cp.wait_recv()


def run_exchange(band_rows, tok, down, up):
    dma = pltpu.SemaphoreType.DMA
    vmem = pl.BlockSpec(memory_space=pltpu.VMEM)
    anywhere = pl.BlockSpec(memory_space=pl.ANY)
    col = (MEMBERS, SLOTS, LEVELS, C)
    row = (MEMBERS, COLS + 2, LEVELS, C)
    return pl.pallas_call(
        exchange,
        out_shape=[
            jax.ShapeDtypeStruct((NZ, 96, 384), BF),
            jax.ShapeDtypeStruct((NZ, 48, 768), BF),
            jax.ShapeDtypeStruct(col, BF),
            jax.ShapeDtypeStruct(col, BF),
            jax.ShapeDtypeStruct(row, BF),
            jax.ShapeDtypeStruct(row, BF),
        ],
        in_specs=[pl.BlockSpec(memory_space=pltpu.SMEM), anywhere, anywhere, anywhere],
        out_specs=[vmem] * 6,
        scratch_shapes=[
            pltpu.VMEM((MEMBERS, SLOTS, COLS, LEVELS, C), BF),
            pltpu.VMEM((MEMBERS, COLS, LEVELS, C), BF),
            pltpu.VMEM((6, 384), BF),
            pltpu.VMEM((3, 768), BF),
            pltpu.VMEM((16, 6, 384), BF),
            pltpu.VMEM((16, 3, 768), BF),
            pltpu.VMEM((96, 384), F32),
            pltpu.VMEM((48, 768), F32),
            dma((3,)), dma((16,)), dma((16,)),
            dma((2, 4, PIECES)), dma((2, 4, PIECES)), dma((NZ,)), dma((NZ,)),
            dma((2,)), dma((2,)), dma((6,)), dma((6,)),
        ],
        compiler_params=pltpu.CompilerParams(collective_id=0, has_side_effects=True),
        name="exchange",
    )(band_rows, tok, down, up)


GROUP = 6


def patches(
    band_ref, tok_hbm, wd, wu, west, east, north, south, dg, ds, ug, us, mix,
    out_hbm, ext, fine, wu4, load_sem, store_sem,
):
    lat = lax.axis_index("lat")
    shift = jnp.minimum(lat, 1)
    live = band_ref[0, 1] - band_ref[0, 0]
    load = pltpu.make_async_copy(
        tok_hbm, ext.at[:, pl.ds(shift, SLOTS), 1 : COLS + 1], load_sem
    )
    load.start()
    for g in range(4):
        wu4[g] = wu[:, C * g : C * (g + 1)]
    ext[:, pl.ds(shift, SLOTS), 0] = west[...]
    ext[:, pl.ds(shift, SLOTS), COLS + 1] = east[...]
    load.wait()

    @pl.when(lat > 0)
    def _():
        ext[:, 0] = north[...]

    ext[:, pl.ds(jnp.clip(live + shift, 0, EXT - 1), 1)] = south[...].reshape(MEMBERS, 1, COLS + 2, LEVELS, C)

    view = ext.reshape(MEMBERS, HALF, 2, 4, 2, LEVELS, C)
    eps = 1e-05
    stores = []
    for m in range(MEMBERS):
        @pl.loop(0, HALF // GROUP)
        def _(it):
            k0 = it * GROUP
            cells = {}
            total = None
            for q in range(2):
                for p in range(2):
                    x = jnp.concatenate(
                        [view[m, pl.ds(k0, GROUP), p, j, q].reshape(GROUP * LEVELS, C) for j in range(4)], axis=0
                    ).astype(F32)
                    cells[q, p] = x
                    s = jnp.sum(x, axis=1, keepdims=True)
                    total = s if total is None else total + s
            average = total * (1.0 / (4 * C))
            total = None
            for key in cells:
                cells[key] = cells[key] - average
                s = jnp.sum(cells[key] * cells[key], axis=1, keepdims=True)
                total = s if total is None else total + s
            scale = lax.rsqrt(total * (1.0 / (4 * C)) + eps)
            coarse = None
            for q in range(2):
                for p in range(2):
                    g = 2 * q + p
                    normed = (cells[q, p] * scale * dg[g : g + 1, :] + ds[g : g + 1, :]).astype(BF)
                    term = jnp.dot(normed, wd[C * g : C * (g + 1), :], preferred_element_type=F32)
                    coarse = term if coarse is None else coarse + term
            coarse = coarse.astype(BF)
            n = GROUP * LEVELS
            for p in range(2):
                for q in range(2):
                    j0 = 1 - q
                    grown = jnp.dot(coarse[n * j0 : n * (j0 + 3)], wu4[2 * p + q], preferred_element_type=F32)
                    average = jnp.sum(grown, axis=1, keepdims=True) * (1.0 / C)
                    grown = grown - average
                    spread = jnp.sum(grown * grown, axis=1, keepdims=True) * (1.0 / C)
                    normed = (grown * lax.rsqrt(spread + eps) * ug[...] + us[...]).astype(BF)
                    done = jnp.dot(normed, mix[...], preferred_element_type=F32).astype(BF)
                    done = done.reshape(3, GROUP, LEVELS, C)
                    rows = 2 * (k0 + lax.broadcasted_iota(jnp.int32, (GROUP, LEVELS, C), 0)) + p
                    keep = rows < live + shift
                    for j in range(3):
                        fine[m, pl.ds(k0, GROUP), p, 2 * (j + j0) + q - 1] = jnp.where(keep, done[j], jnp.zeros_like(done[j]))
        rows_out = fine.reshape(MEMBERS, EXT, COLS, LEVELS, C)
        store = pltpu.make_async_copy(rows_out.at[m, pl.ds(shift, SLOTS)], out_hbm.at[m], store_sem.at[m])
        store.start()
        stores.append(store)
    for store in stores:
        store.wait()


def run_patches(band_rows, tok, wd, wu, west, east, north, south, dg, ds, ug, us, mix):
    vmem = pl.BlockSpec(memory_space=pltpu.VMEM)
    anywhere = pl.BlockSpec(memory_space=pl.ANY)
    return pl.pallas_call(
        patches,
        out_shape=jax.ShapeDtypeStruct((MEMBERS, SLOTS, COLS, LEVELS, C), BF),
        in_specs=[pl.BlockSpec(memory_space=pltpu.SMEM), anywhere] + [vmem] * 11,
        out_specs=anywhere,
        scratch_shapes=[
            pltpu.VMEM((MEMBERS, EXT, COLS + 2, LEVELS, C), BF),
            pltpu.VMEM((MEMBERS, HALF, 2, COLS, LEVELS, C), BF),
            pltpu.VMEM((4, 2 * C, C), BF),
            pltpu.SemaphoreType.DMA,
            pltpu.SemaphoreType.DMA((MEMBERS,)),
        ],
        name="patches",
    )(band_rows, tok, wd, wu, west, east, north, south, dg, ds, ug, us, mix)


def body(
    tokens, band_rows, down_gain, down_shift, down_weight, up_weight, up_gain, up_shift, mix_weight
):
    tok = tokens.transpose(0, 2, 3, 1, 4)
    wd, wu, west, east, north, south = run_exchange(band_rows, tok, down_weight, up_weight)
    out = run_patches(
        band_rows, tok, wd.reshape(4 * C, 2 * C), wu.reshape(2 * C, 4 * C), west, east, north, south,
        down_gain.reshape(4, C), down_shift.reshape(4, C), up_gain.reshape(1, C), up_shift.reshape(1, C), mix_weight,
    )
    return out.transpose(0, 3, 1, 2, 4)


def solution(mesh):
    return jax.shard_map(
        body,
        mesh=mesh,
        in_specs=(
            P("mem", None, "lat", "lon", None),
            P("lat", None),
            P(),
            P(),
            P(("lon", "lat"), None),
            P(("lon", "lat"), None),
            P(),
            P(),
            P(),
        ),
        out_specs=P("mem", None, "lat", "lon", None),
        check_vma=False,
    )
```

```python
import functools

import jax
import jax.numpy as jnp
from jax import lax
from jax.experimental import pallas as pl
from jax.experimental.pallas import tpu as pltpu
from jax.sharding import PartitionSpec as P

MESH = pl.DeviceIdType.MESH
MEMBERS, LEVELS, SLOTS, COLS, C = 2, 8, 34, 6, 192
EXT = SLOTS + 2
HALF = EXT // 2
NZ = 8
PIECES = 3
BF = jnp.bfloat16
F32 = jnp.float32


def exchange(
    band_ref, tok, own_d, own_u,
    wd, wu, west, east, north, south,
    last, got_d, got_u, flat_d, flat_u,
    s1_send, s1_recv, ring_send, ring_recv, pair_send, pair_recv,
    col_send, col_recv, row_send, row_recv,
):
    lon, lat, mem = lax.axis_index("lon"), lax.axis_index("lat"), lax.axis_index("mem")
    z, yh = lon // 2, lon % 2
    core, xx = lat % 2, lat // 2

    def at(lon_, lat_, mem_):
        return (lon_, lat_, mem_)

    def other(yh_):
        return 2 * z + yh_

    lon_w, lon_e = (lon + 15) % 16, (lon + 1) % 16
    lat_n, lat_s = (lat + 7) % 8, (lat + 1) % 8
    up_z = ((z + 1) % NZ) * 2 + yh
    dn_z = ((z + NZ - 1) % NZ) * 2 + yh
    barrier = pltpu.get_barrier_semaphore()

    def greet(where):
        pl.semaphore_signal(barrier, inc=1, device_id=where, device_id_type=MESH)

    for d in range(1, 8):
        greet(at(lon, (lat + d) % 8, mem))
    for d in range(8):
        greet(at(other(1 - yh), (lat + d) % 8, 1 - mem))
    for where in (
        at(up_z, lat, mem), at(dn_z, lat, mem), at(lon_w, lat, mem), at(lon_e, lat, mem),
        at(lon_w, lat_n, mem), at(lon_w, lat_s, mem), at(lon_e, lat_n, mem), at(lon_e, lat_s, mem),
    ):
        greet(where)
    pl.semaphore_wait(barrier, 23)

    me = yh * 8 + lat

    def copy(src, dst, ssem, rsem, where):
        return pltpu.make_async_remote_copy(
            src_ref=src, dst_ref=dst, send_sem=ssem, recv_sem=rsem,
            device_id=where, device_id_type=MESH,
        )

    def stage_one(src, got, kind, base):
        out = []
        for d in range(4):
            lat_t = 2 * ((xx + d) % 4) + kind
            out.append((d, 0, copy(src, got.at[me], s1_send.at[base + d], s1_recv.at[me], at(lon, lat_t, mem))))
            out.append((d, 1, copy(src, got.at[me], s1_send.at[base + 4 + d], s1_recv.at[me], at(other(1 - yh), lat_t, 1 - mem))))
        return out

    sends = [(0, s) for s in stage_one(own_d, got_d, 0, 0)] + [(1, s) for s in stage_one(own_u, got_u, 1, 8)]
    for kind, (d, far, cp) in sends:
        if d == 0 and far == 0:
            @pl.when(core != kind)
            def _():
                cp.start()
        else:
            cp.start()

    cols = [
        copy(tok.at[:, :, 0], east, col_send.at[0], col_recv.at[0], at(lon_w, lat, mem)),
        copy(tok.at[:, :, COLS - 1], west, col_send.at[1], col_recv.at[1], at(lon_e, lat, mem)),
    ]
    for cp in cols:
        cp.start()

    live = band_ref[0, 1] - band_ref[0, 0]
    last[...] = tok[:, pl.ds(jnp.clip(live - 1, 0, SLOTS - 1), 1)].reshape(MEMBERS, COLS, LEVELS, C)
    to_next = [
        copy(last, north.at[:, 1 : COLS + 1], row_send.at[0], row_recv.at[0], at(lon, lat_s, mem)),
        copy(last.at[:, 0], north.at[:, COLS + 1], row_send.at[1], row_recv.at[1], at(lon_w, lat_s, mem)),
        copy(last.at[:, COLS - 1], north.at[:, 0], row_send.at[2], row_recv.at[2], at(lon_e, lat_s, mem)),
    ]
    to_prev = [
        copy(tok.at[:, 0], south.at[:, 1 : COLS + 1], row_send.at[3], row_recv.at[3], at(lon, lat_n, mem)),
        copy(tok.at[:, 0, 0], south.at[:, COLS + 1], row_send.at[4], row_recv.at[4], at(lon_w, lat_n, mem)),
        copy(tok.at[:, 0, COLS - 1], south.at[:, 0], row_send.at[5], row_recv.at[5], at(lon_e, lat_n, mem)),
    ]

    @pl.when(lat < 7)
    def _():
        for cp in to_next:
            cp.start()

    @pl.when(lat > 0)
    def _():
        for cp in to_prev:
            cp.start()

    @pl.when(lat == 7)
    def _():
        south[...] = jnp.zeros_like(south)

    @pl.when(lat == 0)
    def _():
        north[...] = jnp.zeros_like(north)

    def gather(kind, own, got, flat, full, rows):
        part = 16 * rows // PIECES
        got[pl.ds(me, 1)] = own[...].reshape(1, *own.shape)
        for d in range(1, 16):
            i = (me + d) % 16
            copy(own, got.at[i], s1_send.at[0], s1_recv.at[i], at(lon, lat, mem)).wait_recv()
        for i in range(16):
            flat[rows * i : rows * (i + 1), :] = got[i].astype(F32)
        full[pl.ds(z, 1)] = flat[...].astype(BF).reshape(1, *flat.shape)

        def block(step, way):
            return (z + NZ + (step if way else -step)) % NZ

        def piece(b, k):
            return full.at[b, part * k : part * (k + 1)]

        def ring(step, way, k):
            b = block(step, way)
            return copy(
                piece(b, k), piece(b, k), ring_send.at[way, step, k], ring_recv.at[way, step, k],
                at(dn_z if way else up_z, lat, mem),
            )

        def landed(step, way, k):
            b = block(step + 1, way)
            return copy(
                piece(b, k), piece(b, k), ring_send.at[way, step, k], ring_recv.at[way, step, k],
                at(dn_z if way else up_z, lat, mem),
            )

        def pair(b):
            return copy(full.at[b], full.at[b], pair_send.at[b], pair_recv.at[b], at(lon, lat + 1 - 2 * core, mem))

        steps = (4, 3)
        for k in range(PIECES):
            for way in range(2):
                ring(0, way, k).start()
        pair(z).start()
        for step in range(4):
            for k in range(PIECES):
                for way in range(2):
                    if step < steps[way]:
                        landed(step, way, k).wait_recv()
                        if step + 1 < steps[way]:
                            ring(step + 1, way, k).start()
            for way in range(2):
                if step < steps[way]:
                    pair(block(step + 1, way)).start()
        for step in range(4):
            for k in range(PIECES):
                for way in range(2):
                    if step < steps[way]:
                        ring(step, way, k).wait_send()
        for b in range(NZ):
            pair(b).wait_send()

    def take(full):
        for b in range(NZ):
            copy(full.at[b], full.at[b], pair_send.at[b], pair_recv.at[b], at(lon, lat, mem)).wait_recv()

    @pl.when(core == 0)
    def _():
        gather(0, own_d, got_d, flat_d, wd, 6)
        take(wu)

    @pl.when(core == 1)
    def _():
        gather(1, own_u, got_u, flat_u, wu, 3)
        take(wd)

    for kind, (d, far, cp) in sends:
        if d == 0 and far == 0:
            @pl.when(core != kind)
            def _():
                cp.wait_send()
        else:
            cp.wait_send()
    for cp in cols:
        cp.wait()

    @pl.when(lat < 7)
    def _():
        for cp in to_next:
            cp.wait_send()
        for cp in to_prev:
            cp.wait_recv()

    @pl.when(lat > 0)
    def _():
        for cp in to_prev:
            cp.wait_send()
        for cp in to_next:
            cp.wait_recv()


def run_exchange(band_rows, tok, down, up):
    dma = pltpu.SemaphoreType.DMA
    vmem = pl.BlockSpec(memory_space=pltpu.VMEM)
    col = (MEMBERS, SLOTS, LEVELS, C)
    row = (MEMBERS, COLS + 2, LEVELS, C)
    return pl.pallas_call(
        exchange,
        out_shape=[
            jax.ShapeDtypeStruct((NZ, 96, 384), BF),
            jax.ShapeDtypeStruct((NZ, 48, 768), BF),
            jax.ShapeDtypeStruct(col, BF),
            jax.ShapeDtypeStruct(col, BF),
            jax.ShapeDtypeStruct(row, BF),
            jax.ShapeDtypeStruct(row, BF),
        ],
        in_specs=[pl.BlockSpec(memory_space=pltpu.SMEM), vmem, vmem, vmem],
        out_specs=[vmem] * 6,
        scratch_shapes=[
            pltpu.VMEM((MEMBERS, COLS, LEVELS, C), BF),
            pltpu.VMEM((16, 6, 384), BF),
            pltpu.VMEM((16, 3, 768), BF),
            pltpu.VMEM((96, 384), F32),
            pltpu.VMEM((48, 768), F32),
            dma((16,)), dma((16,)),
            dma((2, 4, PIECES)), dma((2, 4, PIECES)), dma((NZ,)), dma((NZ,)),
            dma((2,)), dma((2,)), dma((6,)), dma((6,)),
        ],
        compiler_params=pltpu.CompilerParams(collective_id=0, has_side_effects=True, vmem_limit_bytes=24 << 20),
        name="exchange",
    )(band_rows, tok, down, up)


GROUP = 6


def patches(
    band_ref, tok, wd, wu, west, east, north, south, dg, ds, ug, us, mix,
    out_hbm, ext, fine, wu4, store_sem,
):
    lat = lax.axis_index("lat")
    shift = jnp.minimum(lat, 1)
    live = band_ref[0, 1] - band_ref[0, 0]
    for g in range(4):
        wu4[g] = wu[:, C * g : C * (g + 1)]
    ext[:, pl.ds(shift, SLOTS), 0] = west[...]
    ext[:, pl.ds(shift, SLOTS), COLS + 1] = east[...]
    ext[:, pl.ds(shift, SLOTS), 1 : COLS + 1] = tok[...]

    @pl.when(lat > 0)
    def _():
        ext[:, 0] = north[...]

    ext[:, pl.ds(jnp.clip(live + shift, 0, EXT - 1), 1)] = south[...].reshape(MEMBERS, 1, COLS + 2, LEVELS, C)

    view = ext.reshape(MEMBERS, HALF, 2, 4, 2, LEVELS, C)
    eps = 1e-05
    gains, shifts = dg[...].reshape(1, 4 * C), ds[...].reshape(1, 4 * C)
    fine_gain, fine_shift = ug[...].reshape(1, C), us[...].reshape(1, C)
    stores = []
    for m in range(MEMBERS):
        @pl.loop(0, HALF // GROUP)
        def _(it):
            k0 = it * GROUP
            cells = {}
            total = None
            for q in range(2):
                for p in range(2):
                    x = jnp.concatenate(
                        [view[m, pl.ds(k0, GROUP), p, j, q].reshape(GROUP * LEVELS, C) for j in range(4)], axis=0
                    ).astype(F32)
                    cells[q, p] = x
                    s = jnp.sum(x, axis=1, keepdims=True)
                    total = s if total is None else total + s
            average = total * (1.0 / (4 * C))
            total = None
            for key in cells:
                cells[key] = cells[key] - average
                s = jnp.sum(cells[key] * cells[key], axis=1, keepdims=True)
                total = s if total is None else total + s
            scale = lax.rsqrt(total * (1.0 / (4 * C)) + eps)
            coarse = None
            for q in range(2):
                for p in range(2):
                    g = 2 * q + p
                    normed = (cells[q, p] * scale * gains[:, C * g : C * (g + 1)] + shifts[:, C * g : C * (g + 1)]).astype(BF)
                    term = jnp.dot(normed, wd[C * g : C * (g + 1), :], preferred_element_type=F32)
                    coarse = term if coarse is None else coarse + term
            coarse = coarse.astype(BF)
            n = GROUP * LEVELS
            for p in range(2):
                for q in range(2):
                    j0 = 1 - q
                    grown = jnp.dot(coarse[n * j0 : n * (j0 + 3)], wu4[2 * p + q], preferred_element_type=F32)
                    average = jnp.sum(grown, axis=1, keepdims=True) * (1.0 / C)
                    grown = grown - average
                    spread = jnp.sum(grown * grown, axis=1, keepdims=True) * (1.0 / C)
                    normed = (grown * lax.rsqrt(spread + eps) * fine_gain + fine_shift).astype(BF)
                    done = jnp.dot(normed, mix[...], preferred_element_type=F32).astype(BF)
                    done = done.reshape(3, GROUP, LEVELS, C)
                    rows = 2 * (k0 + lax.broadcasted_iota(jnp.int32, (GROUP, LEVELS, C), 0)) + p
                    keep = rows < live + shift
                    for j in range(3):
                        fine[m, pl.ds(k0, GROUP), p, 2 * (j + j0) + q - 1] = jnp.where(keep, done[j], jnp.zeros_like(done[j]))
        rows_out = fine.reshape(MEMBERS, EXT, COLS, LEVELS, C)
        store = pltpu.make_async_copy(rows_out.at[m, pl.ds(shift, SLOTS)], out_hbm.at[m], store_sem.at[m])
        store.start()
        stores.append(store)
    for store in stores:
        store.wait()


def run_patches(band_rows, tok, wd, wu, west, east, north, south, dg, ds, ug, us, mix):
    vmem = pl.BlockSpec(memory_space=pltpu.VMEM)
    anywhere = pl.BlockSpec(memory_space=pl.ANY)
    return pl.pallas_call(
        patches,
        out_shape=jax.ShapeDtypeStruct((MEMBERS, SLOTS, COLS, LEVELS, C), BF),
        in_specs=[pl.BlockSpec(memory_space=pltpu.SMEM), vmem] + [vmem] * 11,
        out_specs=anywhere,
        scratch_shapes=[
            pltpu.VMEM((MEMBERS, EXT, COLS + 2, LEVELS, C), BF),
            pltpu.VMEM((MEMBERS, HALF, 2, COLS, LEVELS, C), BF),
            pltpu.VMEM((4, 2 * C, C), BF),
            pltpu.SemaphoreType.DMA((MEMBERS,)),
        ],
        compiler_params=pltpu.CompilerParams(vmem_limit_bytes=24 << 20),
        name="patches",
    )(band_rows, tok, wd, wu, west, east, north, south, dg, ds, ug, us, mix)


def body(
    tokens, band_rows, down_gain, down_shift, down_weight, up_weight, up_gain, up_shift, mix_weight
):
    tok = tokens.transpose(0, 2, 3, 1, 4)
    wd, wu, west, east, north, south = run_exchange(band_rows, tok, down_weight, up_weight)
    out = run_patches(
        band_rows, tok, wd.reshape(4 * C, 2 * C), wu.reshape(2 * C, 4 * C), west, east, north, south,
        down_gain, down_shift, up_gain, up_shift, mix_weight,
    )
    return out.transpose(0, 3, 1, 2, 4)


def solution(mesh):
    return jax.shard_map(
        body,
        mesh=mesh,
        in_specs=(
            P("mem", None, "lat", "lon", None),
            P("lat", None),
            P(),
            P(),
            P(("lon", "lat"), None),
            P(("lon", "lat"), None),
            P(),
            P(),
            P(),
        ),
        out_specs=P("mem", None, "lat", "lon", None),
        check_vma=False,
    )
```

```python
import functools

import jax
import jax.numpy as jnp
from jax import lax
from jax.experimental import pallas as pl
from jax.experimental.pallas import tpu as pltpu
from jax.sharding import PartitionSpec as P

MESH = pl.DeviceIdType.MESH
MEMBERS, LEVELS, SLOTS, COLS, C = 2, 8, 34, 6, 192
EXT = SLOTS + 2
HALF = EXT // 2
NZ = 8
ORDER = (4, 3, 5, 2, 6, 1, 7)
ARRIVE = (1, 7, 2, 6, 3, 5, 4)
LAG = 6
BF = jnp.bfloat16
F32 = jnp.float32


def exchange(
    band_hbm, tok_hbm, down_hbm, up_hbm,
    wd, wu, west, east, north, south,
    band_ref, tok, last, own_d, own_u, got_d, got_u, flat_d, flat_u,
    load_sem, s1_send, s1_recv, z_send, z_recv, x_send, x_recv, pair_send, pair_recv,
    col_send, col_recv, row_send, row_recv,
):
    lon, lat, mem = lax.axis_index("lon"), lax.axis_index("lat"), lax.axis_index("mem")
    z, yh = lon // 2, lon % 2
    core, xx = lat % 2, lat // 2
    kind = xx % 2

    loads = [
        pltpu.make_async_copy(down_hbm, own_d, load_sem.at[0]),
        pltpu.make_async_copy(up_hbm, own_u, load_sem.at[1]),
        pltpu.make_async_copy(tok_hbm, tok, load_sem.at[2]),
        pltpu.make_async_copy(band_hbm, band_ref, load_sem.at[3]),
    ]
    for load in loads:
        load.start()

    lon_w, lon_e = (lon + 15) % 16, (lon + 1) % 16
    lat_n, lat_s = (lat + 7) % 8, (lat + 1) % 8
    lon_o, mem_o = 2 * z + 1 - yh, 1 - mem
    mate = (lon, lat + 1 - 2 * core, mem)
    beside = (lon, 2 * ((xx + 1 + 2 * core) % 4) + core, mem)

    def along(d):
        return (2 * ((z + d) % NZ) + yh, lat, mem)

    barrier = pltpu.get_barrier_semaphore()
    partners = [(lon, (lat + d) % 8, mem) for d in range(1, 8)]
    partners += [(lon_o, (lat + d) % 8, mem_o) for d in range(8)]
    partners += [along(d) for d in range(1, NZ)]
    partners += [
        (lon_w, lat, mem), (lon_e, lat, mem),
        (lon_w, lat_n, mem), (lon_w, lat_s, mem), (lon_e, lat_n, mem), (lon_e, lat_s, mem),
    ]
    for where in partners:
        pl.semaphore_signal(barrier, inc=1, device_id=where, device_id_type=MESH)
    for load in loads:
        load.wait()
    live = band_ref[0, 1] - band_ref[0, 0]
    last[...] = tok[:, pl.ds(jnp.clip(live - 1, 0, SLOTS - 1), 1)].reshape(MEMBERS, COLS, LEVELS, C)
    pl.semaphore_wait(barrier, len(partners))

    def copy(src, dst, ssem, rsem, where):
        return pltpu.make_async_remote_copy(
            src_ref=src, dst_ref=dst, send_sem=ssem, recv_sem=rsem,
            device_id=where, device_id_type=MESH,
        )

    firsts = []
    for d in range(2):
        for what, (src, got) in enumerate(((own_d, got_d), (own_u, got_u))):
            lat_t = 2 * ((2 * d + what + 2 * (xx // 2)) % 4) + yh
            i = 4 * d + 2 * what
            firsts.append((lat_t != lat, copy(src, got.at[lat], s1_send.at[i], s1_recv.at[lat], (lon, lat_t, mem))))
            firsts.append((None, copy(src, got.at[lat], s1_send.at[i + 1], s1_recv.at[lat], (lon_o, lat_t, mem_o))))

    def each(op):
        for when, cp in firsts:
            if when is None:
                op(cp)
            else:
                @pl.when(when)
                def _():
                    op(cp)

    each(lambda cp: cp.start())

    to_next = [
        copy(last, north.at[:, 1 : COLS + 1], row_send.at[0], row_recv.at[0], (lon, lat_s, mem)),
        copy(last.at[:, 0], north.at[:, COLS + 1], row_send.at[1], row_recv.at[1], (lon_w, lat_s, mem)),
        copy(last.at[:, COLS - 1], north.at[:, 0], row_send.at[2], row_recv.at[2], (lon_e, lat_s, mem)),
    ]
    to_prev = [
        copy(tok.at[:, 0], south.at[:, 1 : COLS + 1], row_send.at[3], row_recv.at[3], (lon, lat_n, mem)),
        copy(tok.at[:, 0, 0], south.at[:, COLS + 1], row_send.at[4], row_recv.at[4], (lon_w, lat_n, mem)),
        copy(tok.at[:, 0, COLS - 1], south.at[:, 0], row_send.at[5], row_recv.at[5], (lon_e, lat_n, mem)),
    ]

    @pl.when(lat < 7)
    def _():
        for cp in to_next:
            cp.start()

    @pl.when(lat > 0)
    def _():
        for cp in to_prev:
            cp.start()

    @pl.when(lat == 7)
    def _():
        south[...] = jnp.zeros_like(south)

    @pl.when(lat == 0)
    def _():
        north[...] = jnp.zeros_like(north)

    cols = [
        copy(tok.at[:, :, 0], east, col_send.at[0], col_recv.at[0], (lon_w, lat, mem)),
        copy(tok.at[:, :, COLS - 1], west, col_send.at[1], col_recv.at[1], (lon_e, lat, mem)),
    ]

    def gather(own, got, flat, full, rows, other, rows_o):
        span, span_o = 8 * rows, 8 * rows_o
        home = yh == core

        @pl.when(home)
        def _():
            got[pl.ds(lat, 1)] = own[...].reshape(1, *own.shape)

        for i in range(8):
            @pl.when(jnp.logical_not(jnp.logical_and(home, lat == i)))
            def _():
                copy(own, got.at[i], s1_send.at[0], s1_recv.at[i], mate).wait_recv()

        for i in range(8):
            flat[rows * i : rows * (i + 1), :] = got[i].astype(F32)

        def mine(b):
            return full.at[b, pl.ds(pl.multiple_of(core * span, 8), span)]

        def theirs(b):
            return full.at[b, pl.ds(pl.multiple_of((1 - core) * span, 8), span)]

        def cross(b):
            return other.at[b, pl.ds(pl.multiple_of(core * span_o, 8), span_o)]

        def cross_theirs(b):
            return other.at[b, pl.ds(pl.multiple_of((1 - core) * span_o, 8), span_o)]

        full[pl.ds(z, 1), pl.ds(pl.multiple_of(core * span, 8), span), :] = flat[...].astype(BF).reshape(1, *flat.shape)
        order = (0,) + ORDER
        z_out = [copy(mine(z), mine(z), z_send.at[d], z_recv.at[d], along(d)) for d in ORDER]
        for cp in z_out:
            cp.start()
        for cp in cols:
            cp.start()
        started = []

        def pass_on(d):
            b = (z + NZ - d) % NZ
            if d:
                copy(mine(b), mine(b), z_send.at[d], z_recv.at[d], mate).wait_recv()
            for cp in (
                copy(mine(b), mine(b), x_send.at[d], x_recv.at[d], beside),
                copy(mine(b), mine(b), pair_send.at[0, d], pair_recv.at[0, d], mate),
            ):
                cp.start()
                started.append(cp)

        def hand_over(d):
            b = (z + NZ - d) % NZ
            copy(cross(b), cross(b), x_send.at[d], x_recv.at[d], beside).wait_recv()
            cp = copy(cross(b), cross(b), pair_send.at[1, d], pair_recv.at[1, d], mate)
            cp.start()
            started.append(cp)

        arrivals = (0,) + ARRIVE
        for i, d in enumerate(arrivals):
            pass_on(d)
            if i >= LAG:
                hand_over(arrivals[i - LAG])
        for d in arrivals[NZ - LAG :]:
            hand_over(d)
        for d in arrivals:
            b = (z + NZ - d) % NZ
            copy(theirs(b), theirs(b), pair_send.at[0, d], pair_recv.at[0, d], mate).wait_recv()
            copy(cross_theirs(b), cross_theirs(b), pair_send.at[1, d], pair_recv.at[1, d], mate).wait_recv()
        for cp in z_out + started:
            cp.wait_send()

    @pl.when(kind == 0)
    def _():
        gather(own_d, got_d, flat_d, wd, 6, wu, 3)

    @pl.when(kind == 1)
    def _():
        gather(own_u, got_u, flat_u, wu, 3, wd, 6)

    each(lambda cp: cp.wait_send())
    for cp in cols:
        cp.wait()

    @pl.when(lat < 7)
    def _():
        for cp in to_next:
            cp.wait_send()
        for cp in to_prev:
            cp.wait_recv()

    @pl.when(lat > 0)
    def _():
        for cp in to_prev:
            cp.wait_send()
        for cp in to_next:
            cp.wait_recv()


def run_exchange(band_rows, tok, down, up):
    dma = pltpu.SemaphoreType.DMA
    vmem = pl.BlockSpec(memory_space=pltpu.VMEM)
    hbm = pl.BlockSpec(memory_space=pltpu.HBM)
    col = (MEMBERS, SLOTS, LEVELS, C)
    row = (MEMBERS, COLS + 2, LEVELS, C)
    return pl.pallas_call(
        exchange,
        out_shape=[
            jax.ShapeDtypeStruct((NZ, 96, 384), BF),
            jax.ShapeDtypeStruct((NZ, 48, 768), BF),
            jax.ShapeDtypeStruct(col, BF),
            jax.ShapeDtypeStruct(col, BF),
            jax.ShapeDtypeStruct(row, BF),
            jax.ShapeDtypeStruct(row, BF),
        ],
        in_specs=[hbm] * 4,
        out_specs=[vmem] * 6,
        scratch_shapes=[
            pltpu.SMEM((1, 2), jnp.int32),
            pltpu.VMEM((MEMBERS, SLOTS, COLS, LEVELS, C), BF),
            pltpu.VMEM((MEMBERS, COLS, LEVELS, C), BF),
            pltpu.VMEM((6, 384), BF),
            pltpu.VMEM((3, 768), BF),
            pltpu.VMEM((8, 6, 384), BF),
            pltpu.VMEM((8, 3, 768), BF),
            pltpu.VMEM((48, 384), F32),
            pltpu.VMEM((24, 768), F32),
            dma((4,)), dma((8,)), dma((8,)), dma((NZ,)), dma((NZ,)), dma((NZ,)), dma((NZ,)),
            dma((2, NZ)), dma((2, NZ)), dma((2,)), dma((2,)), dma((6,)), dma((6,)),
        ],
        compiler_params=pltpu.CompilerParams(
            collective_id=0, has_side_effects=True, vmem_limit_bytes=24 << 20
        ),
        name="exchange",
    )(*(pltpu.with_memory_space_constraint(v, pltpu.HBM) for v in (band_rows, tok, down, up)))


GROUP = 6


def patches(
    band_ref, tok, wd, wu, west, east, north, south, dg, ds, ug, us, mix_hbm,
    out_hbm, mix, ext, fine, wu4, load_sem, store_sem,
):
    lat = lax.axis_index("lat")
    shift = jnp.minimum(lat, 1)
    live = band_ref[0, 1] - band_ref[0, 0]
    load = pltpu.make_async_copy(mix_hbm, mix, load_sem)
    load.start()
    for g in range(4):
        wu4[g] = wu[:, C * g : C * (g + 1)]
    ext[:, pl.ds(shift, SLOTS), 0] = west[...]
    ext[:, pl.ds(shift, SLOTS), COLS + 1] = east[...]
    ext[:, pl.ds(shift, SLOTS), 1 : COLS + 1] = tok[...]

    @pl.when(lat > 0)
    def _():
        ext[:, 0] = north[...]

    ext[:, pl.ds(jnp.clip(live + shift, 0, EXT - 1), 1)] = south[...].reshape(MEMBERS, 1, COLS + 2, LEVELS, C)

    load.wait()
    view = ext.reshape(MEMBERS, HALF, 2, 4, 2, LEVELS, C)
    eps = 1e-05
    gains, shifts = dg[...].reshape(1, 4 * C), ds[...].reshape(1, 4 * C)
    fine_gain, fine_shift = ug[...].reshape(1, C), us[...].reshape(1, C)
    stores = []
    for m in range(MEMBERS):
        @pl.loop(0, HALF // GROUP)
        def _(it):
            k0 = it * GROUP
            cells = {}
            total = None
            for q in range(2):
                for p in range(2):
                    x = jnp.concatenate(
                        [view[m, pl.ds(k0, GROUP), p, j, q].reshape(GROUP * LEVELS, C) for j in range(4)], axis=0
                    ).astype(F32)
                    cells[q, p] = x
                    s = jnp.sum(x, axis=1, keepdims=True)
                    total = s if total is None else total + s
            average = total * (1.0 / (4 * C))
            total = None
            for key in cells:
                cells[key] = cells[key] - average
                s = jnp.sum(cells[key] * cells[key], axis=1, keepdims=True)
                total = s if total is None else total + s
            scale = lax.rsqrt(total * (1.0 / (4 * C)) + eps)
            coarse = None
            for q in range(2):
                for p in range(2):
                    g = 2 * q + p
                    normed = (cells[q, p] * scale * gains[:, C * g : C * (g + 1)] + shifts[:, C * g : C * (g + 1)]).astype(BF)
                    term = jnp.dot(normed, wd[C * g : C * (g + 1), :], preferred_element_type=F32)
                    coarse = term if coarse is None else coarse + term
            coarse = coarse.astype(BF)
            n = GROUP * LEVELS
            for p in range(2):
                for q in range(2):
                    j0 = 1 - q
                    grown = jnp.dot(coarse[n * j0 : n * (j0 + 3)], wu4[2 * p + q], preferred_element_type=F32)
                    average = jnp.sum(grown, axis=1, keepdims=True) * (1.0 / C)
                    grown = grown - average
                    spread = jnp.sum(grown * grown, axis=1, keepdims=True) * (1.0 / C)
                    normed = (grown * lax.rsqrt(spread + eps) * fine_gain + fine_shift).astype(BF)
                    done = jnp.dot(normed, mix[...], preferred_element_type=F32).astype(BF)
                    done = done.reshape(3, GROUP, LEVELS, C)
                    rows = 2 * (k0 + lax.broadcasted_iota(jnp.int32, (GROUP, LEVELS, C), 0)) + p
                    keep = rows < live + shift
                    for j in range(3):
                        fine[m, pl.ds(k0, GROUP), p, 2 * (j + j0) + q - 1] = jnp.where(keep, done[j], jnp.zeros_like(done[j]))
        rows_out = fine.reshape(MEMBERS, EXT, COLS, LEVELS, C)
        store = pltpu.make_async_copy(rows_out.at[m, pl.ds(shift, SLOTS)], out_hbm.at[m], store_sem.at[m])
        store.start()
        stores.append(store)
    for store in stores:
        store.wait()


def run_patches(band_rows, tok, wd, wu, west, east, north, south, dg, ds, ug, us, mix):
    vmem = pl.BlockSpec(memory_space=pltpu.VMEM)
    anywhere = pl.BlockSpec(memory_space=pl.ANY)
    return pl.pallas_call(
        patches,
        out_shape=jax.ShapeDtypeStruct((MEMBERS, SLOTS, COLS, LEVELS, C), BF),
        in_specs=[pl.BlockSpec(memory_space=pltpu.SMEM), vmem] + [vmem] * 10 + [pl.BlockSpec(memory_space=pltpu.HBM)],
        out_specs=anywhere,
        scratch_shapes=[
            pltpu.VMEM((C, C), BF),
            pltpu.VMEM((MEMBERS, EXT, COLS + 2, LEVELS, C), BF),
            pltpu.VMEM((MEMBERS, HALF, 2, COLS, LEVELS, C), BF),
            pltpu.VMEM((4, 2 * C, C), BF),
            pltpu.SemaphoreType.DMA,
            pltpu.SemaphoreType.DMA((MEMBERS,)),
        ],
        compiler_params=pltpu.CompilerParams(vmem_limit_bytes=24 << 20),
        name="patches",
    )(band_rows, tok, wd, wu, west, east, north, south, dg, ds, ug, us, pltpu.with_memory_space_constraint(mix, pltpu.HBM))


def body(
    tokens, band_rows, down_gain, down_shift, down_weight, up_weight, up_gain, up_shift, mix_weight
):
    tok = tokens.transpose(0, 2, 3, 1, 4)
    wd, wu, west, east, north, south = run_exchange(band_rows, tok, down_weight, up_weight)
    out = run_patches(
        band_rows, tok, wd.reshape(4 * C, 2 * C), wu.reshape(2 * C, 4 * C), west, east, north, south,
        down_gain, down_shift, up_gain, up_shift, mix_weight,
    )
    return out.transpose(0, 3, 1, 2, 4)


def solution(mesh):
    return jax.shard_map(
        body,
        mesh=mesh,
        in_specs=(
            P("mem", None, "lat", "lon", None),
            P("lat", None),
            P(),
            P(),
            P(("lon", "lat"), None),
            P(("lon", "lat"), None),
            P(),
            P(),
            P(),
        ),
        out_specs=P("mem", None, "lat", "lon", None),
        check_vma=False,
    )
```

```python
import functools

import jax
import jax.numpy as jnp
from jax import lax
from jax.experimental import pallas as pl
from jax.experimental.pallas import tpu as pltpu
from jax.sharding import PartitionSpec as P

MESH = pl.DeviceIdType.MESH
MEMBERS, LEVELS, SLOTS, COLS, C = 2, 8, 34, 6, 192
EXT = SLOTS + 2
HALF = EXT // 2
NZ = 8
ORDER = (4, 3, 5, 2, 6, 1, 7)
ARRIVE = (1, 7, 2, 6, 3, 5, 4)
LAG = 6
INSIDE = 0
BF = jnp.bfloat16
F32 = jnp.float32


def exchange(
    band_hbm, tok_hbm, down_hbm, up_hbm, dg_hbm, ds_hbm,
    wd, wu, normed,
    band_ref, dg, ds, tok, west, east, north, south, last, own_d, own_u, got_d, got_u, flat_d, flat_u,
    load_sem, s1_send, s1_recv, z_send, z_recv, x_send, x_recv, pair_send, pair_recv,
    col_send, col_recv, row_send, row_recv,
):
    lon, lat, mem = lax.axis_index("lon"), lax.axis_index("lat"), lax.axis_index("mem")
    z, yh = lon // 2, lon % 2
    core, xx = lat % 2, lat // 2
    kind = xx % 2
    shift = jnp.minimum(lat, 1)

    loads = [
        pltpu.make_async_copy(down_hbm, own_d, load_sem.at[0]),
        pltpu.make_async_copy(up_hbm, own_u, load_sem.at[1]),
        pltpu.make_async_copy(tok_hbm, tok.at[:, pl.ds(shift, SLOTS)], load_sem.at[2]),
        pltpu.make_async_copy(band_hbm, band_ref, load_sem.at[3]),
        pltpu.make_async_copy(dg_hbm, dg, load_sem.at[4]),
        pltpu.make_async_copy(ds_hbm, ds, load_sem.at[5]),
    ]
    for load in loads:
        load.start()

    lon_w, lon_e = (lon + 15) % 16, (lon + 1) % 16
    lat_n, lat_s = (lat + 7) % 8, (lat + 1) % 8
    lon_o, mem_o = 2 * z + 1 - yh, 1 - mem
    mate = (lon, lat + 1 - 2 * core, mem)
    beside = (lon, 2 * ((xx + 1 + 2 * core) % 4) + core, mem)

    def along(d):
        return (2 * ((z + d) % NZ) + yh, lat, mem)

    barrier = pltpu.get_barrier_semaphore()
    partners = [(lon, (lat + d) % 8, mem) for d in range(1, 8)]
    partners += [(lon_o, (lat + d) % 8, mem_o) for d in range(8)]
    partners += [along(d) for d in range(1, NZ)]
    partners += [
        (lon_w, lat, mem), (lon_e, lat, mem),
        (lon_w, lat_n, mem), (lon_w, lat_s, mem), (lon_e, lat_n, mem), (lon_e, lat_s, mem),
    ]
    for where in partners:
        pl.semaphore_signal(barrier, inc=1, device_id=where, device_id_type=MESH)
    for load in loads:
        load.wait()
    live = band_ref[0, 1] - band_ref[0, 0]
    last[...] = tok[:, pl.ds(jnp.clip(live - 1, 0, SLOTS - 1) + shift, 1)].reshape(MEMBERS, COLS, LEVELS, C)
    pl.semaphore_wait(barrier, len(partners))

    def copy(src, dst, ssem, rsem, where):
        return pltpu.make_async_remote_copy(
            src_ref=src, dst_ref=dst, send_sem=ssem, recv_sem=rsem,
            device_id=where, device_id_type=MESH,
        )

    firsts = []
    for d in range(2):
        for what, (src, got) in enumerate(((own_d, got_d), (own_u, got_u))):
            lat_t = 2 * ((2 * d + what + 2 * (xx // 2)) % 4) + yh
            i = 4 * d + 2 * what
            firsts.append((lat_t != lat, copy(src, got.at[lat], s1_send.at[i], s1_recv.at[lat], (lon, lat_t, mem))))
            firsts.append((None, copy(src, got.at[lat], s1_send.at[i + 1], s1_recv.at[lat], (lon_o, lat_t, mem_o))))

    def each(op):
        for when, cp in firsts:
            if when is None:
                op(cp)
            else:
                @pl.when(when)
                def _():
                    op(cp)

    each(lambda cp: cp.start())

    to_next = [
        copy(last, north.at[:, 1 : COLS + 1], row_send.at[0], row_recv.at[0], (lon, lat_s, mem)),
        copy(last.at[:, 0], north.at[:, COLS + 1], row_send.at[1], row_recv.at[1], (lon_w, lat_s, mem)),
        copy(last.at[:, COLS - 1], north.at[:, 0], row_send.at[2], row_recv.at[2], (lon_e, lat_s, mem)),
    ]
    to_prev = [
        copy(tok.at[:, shift], south.at[:, 1 : COLS + 1], row_send.at[3], row_recv.at[3], (lon, lat_n, mem)),
        copy(tok.at[:, shift, 0], south.at[:, COLS + 1], row_send.at[4], row_recv.at[4], (lon_w, lat_n, mem)),
        copy(tok.at[:, shift, COLS - 1], south.at[:, 0], row_send.at[5], row_recv.at[5], (lon_e, lat_n, mem)),
    ]

    @pl.when(lat < 7)
    def _():
        for cp in to_next:
            cp.start()

    @pl.when(lat > 0)
    def _():
        for cp in to_prev:
            cp.start()

    @pl.when(lat == 7)
    def _():
        south[...] = jnp.zeros_like(south)

    @pl.when(lat == 0)
    def _():
        north[...] = jnp.zeros_like(north)

    cols = [
        copy(tok.at[:, pl.ds(shift, SLOTS), 0], east.at[:, pl.ds(shift, SLOTS)], col_send.at[0], col_recv.at[0], (lon_w, lat, mem)),
        copy(tok.at[:, pl.ds(shift, SLOTS), COLS - 1], west.at[:, pl.ds(shift, SLOTS)], col_send.at[1], col_recv.at[1], (lon_e, lat, mem)),
    ]

    spot = (live + shift) // 2
    gains, shifts = dg[...].reshape(1, 4 * C), ds[...].reshape(1, 4 * C)

    def cell(m, j, q, p):
        i = 2 * j + q
        if i == 0:
            x = west.reshape(MEMBERS, HALF, 2, LEVELS, C)[m, :, p]
        elif i == COLS + 1:
            x = east.reshape(MEMBERS, HALF, 2, LEVELS, C)[m, :, p]
        else:
            x = tok.reshape(MEMBERS, HALF, 2, COLS, LEVELS, C)[m, :, p, i - 1]
        if p:
            here = lax.broadcasted_iota(jnp.int32, (HALF, LEVELS, C), 0) == spot
            x = jnp.where(here, south[m, i].reshape(1, LEVELS, C), x)
        return x.reshape(HALF * LEVELS, C).astype(F32)

    def norm(j):
        @pl.loop(0, MEMBERS)
        def _(m):
            cells = {(q, p): cell(m, j, q, p) for q in range(2) for p in range(2)}
            total = sum(jnp.sum(x, axis=1, keepdims=True) for x in cells.values())
            average = total * (1.0 / (4 * C))
            cells = {key: x - average for key, x in cells.items()}
            total = sum(jnp.sum(x * x, axis=1, keepdims=True) for x in cells.values())
            scale = lax.rsqrt(total * (1.0 / (4 * C)) + 1e-05)
            for (q, p), x in cells.items():
                g = 2 * q + p
                y = x * scale * gains[:, C * g : C * (g + 1)] + shifts[:, C * g : C * (g + 1)]
                normed[g, j, m] = y.astype(BF)

    def inside():
        @pl.when(lat < 7)
        def _():
            for cp in to_prev:
                cp.wait_recv()

        @pl.when(lat > 0)
        def _():
            for cp in to_next:
                cp.wait_recv()
            tok[:, 0] = north[:, 1 : COLS + 1]

        norm(1)
        norm(2)

    def border():
        for cp in cols:
            cp.wait_recv()

        @pl.when(lat > 0)
        def _():
            west[:, 0] = north[:, 0]
            east[:, 0] = north[:, COLS + 1]

        norm(0)
        norm(3)

    def gather(own, got, flat, full, rows, other, rows_o):
        span, span_o = 8 * rows, 8 * rows_o
        home = yh == core

        @pl.when(home)
        def _():
            got[pl.ds(lat, 1)] = own[...].reshape(1, *own.shape)

        for i in range(8):
            @pl.when(jnp.logical_not(jnp.logical_and(home, lat == i)))
            def _():
                copy(own, got.at[i], s1_send.at[0], s1_recv.at[i], mate).wait_recv()

        for i in range(8):
            flat[rows * i : rows * (i + 1), :] = got[i].astype(F32)

        def mine(b):
            return full.at[b, pl.ds(pl.multiple_of(core * span, 8), span)]

        def theirs(b):
            return full.at[b, pl.ds(pl.multiple_of((1 - core) * span, 8), span)]

        def cross(b):
            return other.at[b, pl.ds(pl.multiple_of(core * span_o, 8), span_o)]

        def cross_theirs(b):
            return other.at[b, pl.ds(pl.multiple_of((1 - core) * span_o, 8), span_o)]

        full[pl.ds(z, 1), pl.ds(pl.multiple_of(core * span, 8), span), :] = flat[...].astype(BF).reshape(1, *flat.shape)
        order = (0,) + ORDER
        z_out = [copy(mine(z), mine(z), z_send.at[d], z_recv.at[d], along(d)) for d in ORDER]
        for cp in z_out:
            cp.start()
        for cp in cols:
            cp.start()
        started = []

        def pass_on(d):
            b = (z + NZ - d) % NZ
            if d:
                copy(mine(b), mine(b), z_send.at[d], z_recv.at[d], mate).wait_recv()
            for cp in (
                copy(mine(b), mine(b), x_send.at[d], x_recv.at[d], beside),
                copy(mine(b), mine(b), pair_send.at[0, d], pair_recv.at[0, d], mate),
            ):
                cp.start()
                started.append(cp)

        def hand_over(d):
            b = (z + NZ - d) % NZ
            copy(cross(b), cross(b), x_send.at[d], x_recv.at[d], beside).wait_recv()
            cp = copy(cross(b), cross(b), pair_send.at[1, d], pair_recv.at[1, d], mate)
            cp.start()
            started.append(cp)

        arrivals = (0,) + ARRIVE
        for i, d in enumerate(arrivals):
            pass_on(d)
            if i == INSIDE:
                inside()
            if i >= LAG:
                hand_over(arrivals[i - LAG])
        for d in arrivals[NZ - LAG :]:
            hand_over(d)
        border()
        for d in arrivals:
            b = (z + NZ - d) % NZ
            copy(theirs(b), theirs(b), pair_send.at[0, d], pair_recv.at[0, d], mate).wait_recv()
            copy(cross_theirs(b), cross_theirs(b), pair_send.at[1, d], pair_recv.at[1, d], mate).wait_recv()
        for cp in z_out + started:
            cp.wait_send()

    @pl.when(kind == 0)
    def _():
        gather(own_d, got_d, flat_d, wd, 6, wu, 3)

    @pl.when(kind == 1)
    def _():
        gather(own_u, got_u, flat_u, wu, 3, wd, 6)

    each(lambda cp: cp.wait_send())
    for cp in cols:
        cp.wait_send()

    @pl.when(lat < 7)
    def _():
        for cp in to_next:
            cp.wait_send()

    @pl.when(lat > 0)
    def _():
        for cp in to_prev:
            cp.wait_send()


def run_exchange(band_rows, tok, down, up, dg, ds):
    dma = pltpu.SemaphoreType.DMA
    vmem = pl.BlockSpec(memory_space=pltpu.VMEM)
    hbm = pl.BlockSpec(memory_space=pltpu.HBM)
    col = (MEMBERS, EXT, LEVELS, C)
    row = (MEMBERS, COLS + 2, LEVELS, C)
    return pl.pallas_call(
        exchange,
        out_shape=[
            jax.ShapeDtypeStruct((NZ, 96, 384), BF),
            jax.ShapeDtypeStruct((NZ, 48, 768), BF),
            jax.ShapeDtypeStruct((4, 4, MEMBERS, HALF * LEVELS, C), BF),
        ],
        in_specs=[hbm] * 6,
        out_specs=[vmem] * 3,
        scratch_shapes=[
            pltpu.SMEM((1, 2), jnp.int32),
            pltpu.VMEM((4 * C,), F32),
            pltpu.VMEM((4 * C,), F32),
            pltpu.VMEM((MEMBERS, EXT, COLS, LEVELS, C), BF),
            pltpu.VMEM(col, BF),
            pltpu.VMEM(col, BF),
            pltpu.VMEM(row, BF),
            pltpu.VMEM(row, BF),
            pltpu.VMEM((MEMBERS, COLS, LEVELS, C), BF),
            pltpu.VMEM((6, 384), BF),
            pltpu.VMEM((3, 768), BF),
            pltpu.VMEM((8, 6, 384), BF),
            pltpu.VMEM((8, 3, 768), BF),
            pltpu.VMEM((48, 384), F32),
            pltpu.VMEM((24, 768), F32),
            dma((6,)), dma((8,)), dma((8,)), dma((NZ,)), dma((NZ,)), dma((NZ,)), dma((NZ,)),
            dma((2, NZ)), dma((2, NZ)), dma((2,)), dma((2,)), dma((6,)), dma((6,)),
        ],
        compiler_params=pltpu.CompilerParams(
            collective_id=0, has_side_effects=True, vmem_limit_bytes=24 << 20
        ),
        name="exchange",
    )(*(pltpu.with_memory_space_constraint(v, pltpu.HBM) for v in (band_rows, tok, down, up, dg, ds)))


SPLIT = ((0, 1),)
ROWS = HALF * LEVELS


def patches(
    band_hbm, wd, wu, normed, ug, us, mix_hbm,
    out_hbm, band_ref, mix, fine, wu4, load_sem, store_sem,
):
    lat = lax.axis_index("lat")
    shift = jnp.minimum(lat, 1)
    loads = [
        pltpu.make_async_copy(mix_hbm, mix, load_sem.at[0]),
        pltpu.make_async_copy(band_hbm, band_ref, load_sem.at[1]),
    ]
    for load in loads:
        load.start()
    for g in range(4):
        wu4[g] = wu[:, C * g : C * (g + 1)]
    eps = 1e-05
    fine_gain, fine_shift = ug[...].reshape(1, C), us[...].reshape(1, C)
    rows_out = fine.reshape(MEMBERS, EXT, COLS, LEVELS, C)
    stores = []
    for members in SPLIT:
        def pick(g):
            return jnp.concatenate([normed[g, j, m] for j in range(4) for m in members], axis=0)

        coarse = None
        for g in range(4):
            term = jnp.dot(pick(g), wd[C * g : C * (g + 1), :], preferred_element_type=F32)
            coarse = term if coarse is None else coarse + term
        coarse = coarse.astype(BF)
        if members == SPLIT[0]:
            for load in loads:
                load.wait()
            bound = band_ref[0, 1] - band_ref[0, 0] + shift
        n = ROWS * len(members)
        for p in range(2):
            keep = 2 * lax.broadcasted_iota(jnp.int32, (HALF, LEVELS, C), 0) + p < bound
            for q in range(2):
                j0 = 1 - q
                grown = jnp.dot(coarse[n * j0 : n * (j0 + 3)], wu4[2 * p + q], preferred_element_type=F32)
                average = jnp.sum(grown, axis=1, keepdims=True) * (1.0 / C)
                grown = grown - average
                spread = jnp.sum(grown * grown, axis=1, keepdims=True) * (1.0 / C)
                unit = (grown * lax.rsqrt(spread + eps) * fine_gain + fine_shift).astype(BF)
                done = jnp.dot(unit, mix[...], preferred_element_type=F32).astype(BF)
                done = done.reshape(3, len(members), HALF, LEVELS, C)
                for j in range(3):
                    for i, m in enumerate(members):
                        fine[m, :, p, 2 * (j + j0) + q - 1] = jnp.where(keep, done[j, i], jnp.zeros_like(done[j, i]))
        for m in members:
            store = pltpu.make_async_copy(rows_out.at[m, pl.ds(shift, SLOTS)], out_hbm.at[m], store_sem.at[m])
            store.start()
            stores.append(store)
    for store in stores:
        store.wait()


def run_patches(band_rows, wd, wu, normed, ug, us, mix):
    vmem = pl.BlockSpec(memory_space=pltpu.VMEM)
    hbm = pl.BlockSpec(memory_space=pltpu.HBM)
    band_rows, mix = (pltpu.with_memory_space_constraint(v, pltpu.HBM) for v in (band_rows, mix))
    return pl.pallas_call(
        patches,
        out_shape=jax.ShapeDtypeStruct((MEMBERS, SLOTS, COLS, LEVELS, C), BF),
        in_specs=[hbm] + [vmem] * 5 + [hbm],
        out_specs=pl.BlockSpec(memory_space=pl.ANY),
        scratch_shapes=[
            pltpu.SMEM((1, 2), jnp.int32),
            pltpu.VMEM((C, C), BF),
            pltpu.VMEM((MEMBERS, HALF, 2, COLS, LEVELS, C), BF),
            pltpu.VMEM((4, 2 * C, C), BF),
            pltpu.SemaphoreType.DMA((2,)),
            pltpu.SemaphoreType.DMA((MEMBERS,)),
        ],
        compiler_params=pltpu.CompilerParams(vmem_limit_bytes=24 << 20),
        name="patches",
    )(band_rows, wd, wu, normed, ug, us, mix)


def body(
    tokens, band_rows, down_gain, down_shift, down_weight, up_weight, up_gain, up_shift, mix_weight
):
    tok = tokens.transpose(0, 2, 3, 1, 4)
    wd, wu, normed = run_exchange(band_rows, tok, down_weight, up_weight, down_gain, down_shift)
    out = run_patches(
        band_rows, wd.reshape(4 * C, 2 * C), wu.reshape(2 * C, 4 * C), normed, up_gain, up_shift, mix_weight
    )
    return out.transpose(0, 3, 1, 2, 4)


def solution(mesh):
    return jax.shard_map(
        body,
        mesh=mesh,
        in_specs=(
            P("mem", None, "lat", "lon", None),
            P("lat", None),
            P(),
            P(),
            P(("lon", "lat"), None),
            P(("lon", "lat"), None),
            P(),
            P(),
            P(),
        ),
        out_specs=P("mem", None, "lat", "lon", None),
        check_vma=False,
    )
```

```python
import functools

import jax
import jax.numpy as jnp
from jax import lax
from jax.experimental import pallas as pl
from jax.experimental.pallas import tpu as pltpu
from jax.sharding import PartitionSpec as P

MESH = pl.DeviceIdType.MESH
MEMBERS, LEVELS, SLOTS, COLS, C = 2, 8, 34, 6, 192
EXT = SLOTS + 2
HALF = EXT // 2
NZ = 8
ORDER = (1, 7, 2, 6, 3, 5, 4)
ARRIVE = (1, 7, 2, 6, 3, 5, 4)
LAG = 6
INSIDE = 0
COLS_AT = (-1, -1)
MIX = 0
BF = jnp.bfloat16
F32 = jnp.float32


def exchange(
    band_hbm, tok_hbm, down_hbm, up_hbm, dg_hbm, ds_hbm,
    wd, wu, normed,
    band_ref, dg, ds, tok, first_col, last_col, west, east, north, south, last, own_d, own_u, got_d, got_u, flat,
    load_sem, s1_send, s1_recv, z_send, z_recv, x_send, x_recv, pair_send, pair_recv,
    col_send, col_recv, row_send, row_recv,
):
    lon, lat, mem = lax.axis_index("lon"), lax.axis_index("lat"), lax.axis_index("mem")
    z, yh = lon // 2, lon % 2
    core, xx = lat % 2, lat // 2
    quarter = (xx + 2 * mem * MIX) % 4
    cy, ch = quarter % 2, quarter // 2
    shift = jnp.minimum(lat, 1)

    loads = [
        pltpu.make_async_copy(down_hbm, own_d, load_sem.at[0]),
        pltpu.make_async_copy(up_hbm, own_u, load_sem.at[1]),
        pltpu.make_async_copy(tok_hbm, tok.at[:, pl.ds(shift, SLOTS)], load_sem.at[2]),
        pltpu.make_async_copy(band_hbm, band_ref, load_sem.at[3]),
        pltpu.make_async_copy(dg_hbm, dg, load_sem.at[4]),
        pltpu.make_async_copy(ds_hbm, ds, load_sem.at[5]),
    ]
    for load in loads:
        load.start()

    @pl.when(lat > 0)
    def _():
        tok[:, 0] = jnp.zeros((MEMBERS, COLS, LEVELS, C), BF)
        tok[:, EXT - 1] = jnp.zeros((MEMBERS, COLS, LEVELS, C), BF)

    @pl.when(lat == 0)
    def _():
        tok[:, SLOTS:] = jnp.zeros((MEMBERS, 2, COLS, LEVELS, C), BF)

    lon_w, lon_e = (lon + 15) % 16, (lon + 1) % 16
    lat_n, lat_s = (lat + 7) % 8, (lat + 1) % 8
    lon_o, mem_o = 2 * z + 1 - yh, 1 - mem
    mate = (lon, lat + 1 - 2 * core, mem)

    def along(d):
        return (2 * ((z + d) % NZ) + yh, lat, mem)

    def across(s):
        return (lon, (lat + 2 * s) % 8, mem)

    barrier = pltpu.get_barrier_semaphore()
    partners = [(lon, (lat + d) % 8, mem) for d in range(1, 8)]
    partners += [(lon_o, (lat + d) % 8, mem_o) for d in range(8)]
    partners += [along(d) for d in range(1, NZ)]
    partners += [(lon, lat, mem_o)]
    partners += [
        (lon_w, lat, mem), (lon_e, lat, mem),
        (lon_w, lat_n, mem), (lon_w, lat_s, mem), (lon_e, lat_n, mem), (lon_e, lat_s, mem),
    ]
    for where in partners:
        pl.semaphore_signal(barrier, inc=1, device_id=where, device_id_type=MESH)
    loads[0].wait()
    loads[1].wait()
    pl.semaphore_wait(barrier, len(partners))

    def copy(src, dst, ssem, rsem, where):
        return pltpu.make_async_remote_copy(
            src_ref=src, dst_ref=dst, send_sem=ssem, recv_sem=rsem,
            device_id=where, device_id_type=MESH,
        )

    firsts = []

    def first(src, dst, i, slot, k, kind):
        lat_t = 2 * ((k + 2 * mem * MIX) % 4) + kind
        lat_f = 2 * ((k + 2 * mem_o * MIX) % 4) + kind
        firsts.append((lat_t != lat, copy(src, dst, s1_send.at[i], s1_recv.at[slot], (lon, lat_t, mem))))
        firsts.append((None, copy(src, dst, s1_send.at[i + 1], s1_recv.at[slot], (lon_o, lat_f, mem_o))))

    first(own_d, got_d.at[lat % 4], 0, lat % 4, yh + 2 * (lat // 4), 0)
    for h in range(2):
        first(own_u.at[:, 384 * h : 384 * (h + 1)], got_u.at[lat], 2 + 2 * h, lat, yh + 2 * h, 1)

    def each(op):
        for when, cp in firsts:
            if when is None:
                op(cp)
            else:
                @pl.when(when)
                def _():
                    op(cp)

    each(lambda cp: cp.start())

    for load in loads[2:]:
        load.wait()
    live = band_ref[0, 1] - band_ref[0, 0]
    last[...] = tok[:, pl.ds(jnp.clip(live - 1, 0, SLOTS - 1) + shift, 1)].reshape(MEMBERS, COLS, LEVELS, C)
    halves = tok.reshape(MEMBERS, HALF, 2, COLS, LEVELS, C)
    for m in range(MEMBERS):
        for i, box in ((0, first_col), (COLS - 1, last_col)):
            a, b = halves[m, :, 0, i], halves[m, :, 1, i]
            box[m, :, 0] = a[:, :, :128]
            box[m, :, 1] = b[:, :, :128]
            box[m, :, 2] = jnp.concatenate([a[:, :, 128:], b[:, :, 128:]], axis=2)

    cols = [
        [
            copy(first_col.at[m], east.at[m], col_send.at[m, 0], col_recv.at[m, 0], (lon_w, lat, mem)),
            copy(last_col.at[m], west.at[m], col_send.at[m, 1], col_recv.at[m, 1], (lon_e, lat, mem)),
        ]
        for m in range(MEMBERS)
    ]
    def start_cols(far):
        for m in range(MEMBERS):
            @pl.when(yh == far)
            def _():
                cols[m][1].start()

            @pl.when(yh != far)
            def _():
                cols[m][0].start()

    for far in range(2):
        if COLS_AT[far] == -2:
            start_cols(far)

    to_next = [
        copy(last, north.at[:, 1 : COLS + 1], row_send.at[0], row_recv.at[0], (lon, lat_s, mem)),
        copy(last.at[:, 0], north.at[:, COLS + 1], row_send.at[1], row_recv.at[1], (lon_w, lat_s, mem)),
        copy(last.at[:, COLS - 1], north.at[:, 0], row_send.at[2], row_recv.at[2], (lon_e, lat_s, mem)),
    ]
    to_prev = [
        copy(tok.at[:, shift], south.at[:, 1 : COLS + 1], row_send.at[3], row_recv.at[3], (lon, lat_n, mem)),
        copy(tok.at[:, shift, 0], south.at[:, COLS + 1], row_send.at[4], row_recv.at[4], (lon_w, lat_n, mem)),
        copy(tok.at[:, shift, COLS - 1], south.at[:, 0], row_send.at[5], row_recv.at[5], (lon_e, lat_n, mem)),
    ]

    @pl.when(lat < 7)
    def _():
        for cp in to_next:
            cp.start()

    @pl.when(lat > 0)
    def _():
        for cp in to_prev:
            cp.start()

    @pl.when(lat == 7)
    def _():
        south[...] = jnp.zeros_like(south)

    @pl.when(lat == 0)
    def _():
        north[...] = jnp.zeros_like(north)

    spot = (live + shift) // 2
    gains, shifts = dg[...].reshape(1, 4 * C), ds[...].reshape(1, 4 * C)

    def cell(m, j, q, p):
        i = 2 * j + q
        where = lax.broadcasted_iota(jnp.int32, (HALF, LEVELS, C), 0)
        if i in (0, COLS + 1):
            box = east if i else west
            x = jnp.concatenate([box[m, :, p], box[m, :, 2][:, :, 64 * p : 64 * p + 64]], axis=2)
            if p == 0:
                x = jnp.where(where + 1 == shift, north[m, i].reshape(1, LEVELS, C), x)
        else:
            x = tok.reshape(MEMBERS, HALF, 2, COLS, LEVELS, C)[m, :, p, i - 1]
        if p:
            x = jnp.where(where == spot, south[m, i].reshape(1, LEVELS, C), x)
        return x.reshape(HALF * LEVELS, C).astype(F32)

    def norm(j):
        @pl.loop(0, MEMBERS)
        def _(m):
            cells = {(q, p): cell(m, j, q, p) for q in range(2) for p in range(2)}
            total = sum(jnp.sum(x, axis=1, keepdims=True) for x in cells.values())
            average = total * (1.0 / (4 * C))
            cells = {key: x - average for key, x in cells.items()}
            total = sum(jnp.sum(x * x, axis=1, keepdims=True) for x in cells.values())
            scale = lax.rsqrt(total * (1.0 / (4 * C)) + 1e-05)
            for (q, p), x in cells.items():
                g = 2 * q + p
                y = x * scale * gains[:, C * g : C * (g + 1)] + shifts[:, C * g : C * (g + 1)]
                normed[g, j, m] = y.astype(BF)

    def inside():
        @pl.when(lat < 7)
        def _():
            for cp in to_prev:
                cp.wait_recv()

        @pl.when(lat > 0)
        def _():
            for cp in to_next:
                cp.wait_recv()
            tok[:, 0] = north[:, 1 : COLS + 1]

        norm(1)
        norm(2)

    def border():
        for cp in cols[0] + cols[1]:
            cp.wait_recv()
        norm(0)
        norm(3)

    def gather(home, parts, keep, got, flat, rows, full, mine):
        count = 24 // rows

        @pl.when(home)
        def _():
            keep()

        for i in range(count):
            @pl.when(jnp.logical_not(jnp.logical_and(home, lat % count == i)))
            def _():
                copy(parts, got.at[i], s1_send.at[0], s1_recv.at[i], mate).wait_recv()

        for i in range(count):
            flat[rows * i : rows * (i + 1), :] = got[i].astype(F32)
        mine(z)[...] = flat[...].astype(BF).reshape(1, 24, 384)
        z_out = [copy(mine(z), mine(z), z_send.at[d], z_recv.at[d], along(d)) for d in ORDER]
        for cp in z_out:
            cp.start()
        for far in range(2):
            if COLS_AT[far] == -1:
                start_cols(far)
        started = []

        def pass_on(b, t):
            part = mine(b)
            for s in range(2):
                cp = copy(part, part, x_send.at[s, t], x_recv.at[s, t], across(1 + 2 * s))
                cp.start()
                started.append(cp)
            side = b % 2
            cp = copy(part, part, x_send.at[2, t], x_recv.at[2, t], (lon + side * (lon_o - lon), lat, mem_o) if MIX else across(2))
            cp.start()
            started.append(cp)

        def hand_over(b, t):
            part = mine(b)
            for s in range(3):
                copy(part, part, x_send.at[s, t], x_recv.at[s, t], mate).wait_recv()
            whole = full.at[b]
            cp = copy(whole, whole, pair_send.at[t], pair_recv.at[t], mate)
            cp.start()
            started.append(cp)

        blocks = [(z + NZ - d) % NZ for d in (0,) + ARRIVE]
        for t, d in enumerate((0,) + ARRIVE):
            if d:
                copy(mine(z), mine(z), z_send.at[d], z_recv.at[d], mate).wait_recv()
            pass_on(blocks[t], t)
            for far in range(2):
                if COLS_AT[far] == t:
                    start_cols(far)
            if t == INSIDE:
                inside()
            if t >= LAG:
                hand_over(blocks[t - LAG], t - LAG)
        for t in range(NZ - LAG, NZ):
            hand_over(blocks[t], t)
        border()
        return z_out + started

    def take(other):
        for t, d in enumerate((0,) + ARRIVE):
            whole = other.at[(z + NZ - d) % NZ]
            copy(whole, whole, pair_send.at[t], pair_recv.at[t], mate).wait_recv()

    @pl.when(core == 0)
    def _():
        def keep():
            got_d[pl.ds(lat % 4, 1)] = own_d[...].reshape(1, 6, 384)

        def mine(b, n=1):
            return wd.at[pl.ds(b, n), pl.ds(pl.multiple_of(48 * cy + 24 * ch, 8), 24)]

        sent = gather(jnp.logical_and(yh == cy, lat // 4 == ch), own_d, keep, got_d, flat, 6, wd, mine)
        take(wu)
        for cp in sent:
            cp.wait_send()

    @pl.when(core == 1)
    def _():
        def keep():
            got_u[pl.ds(lat, 1)] = own_u[:, pl.ds(pl.multiple_of(384 * ch, 128), 384)].reshape(1, 3, 384)

        def mine(b, n=1):
            return wu.at[pl.ds(b, n), pl.ds(pl.multiple_of(24 * cy, 8), 24), pl.ds(pl.multiple_of(384 * ch, 128), 384)]

        sent = gather(yh == cy, own_u.at[:, :384], keep, got_u, flat, 3, wu, mine)
        take(wd)
        for cp in sent:
            cp.wait_send()

    each(lambda cp: cp.wait_send())
    for cp in cols[0] + cols[1]:
        cp.wait_send()

    @pl.when(lat < 7)
    def _():
        for cp in to_next:
            cp.wait_send()

    @pl.when(lat > 0)
    def _():
        for cp in to_prev:
            cp.wait_send()


def run_exchange(band_rows, tok, down, up, dg, ds):
    dma = pltpu.SemaphoreType.DMA
    vmem = pl.BlockSpec(memory_space=pltpu.VMEM)
    hbm = pl.BlockSpec(memory_space=pltpu.HBM)
    col = (MEMBERS, HALF, 3, LEVELS, 128)
    row = (MEMBERS, COLS + 2, LEVELS, C)
    return pl.pallas_call(
        exchange,
        out_shape=[
            jax.ShapeDtypeStruct((NZ, 96, 384), BF),
            jax.ShapeDtypeStruct((NZ, 48, 768), BF),
            jax.ShapeDtypeStruct((4, 4, MEMBERS, HALF * LEVELS, C), BF),
        ],
        in_specs=[hbm] * 6,
        out_specs=[vmem] * 3,
        scratch_shapes=[
            pltpu.SMEM((1, 2), jnp.int32),
            pltpu.VMEM((4 * C,), F32),
            pltpu.VMEM((4 * C,), F32),
            pltpu.VMEM((MEMBERS, EXT, COLS, LEVELS, C), BF),
            pltpu.VMEM(col, BF),
            pltpu.VMEM(col, BF),
            pltpu.VMEM(col, BF),
            pltpu.VMEM(col, BF),
            pltpu.VMEM(row, BF),
            pltpu.VMEM(row, BF),
            pltpu.VMEM((MEMBERS, COLS, LEVELS, C), BF),
            pltpu.VMEM((6, 384), BF),
            pltpu.VMEM((3, 768), BF),
            pltpu.VMEM((4, 6, 384), BF),
            pltpu.VMEM((8, 3, 384), BF),
            pltpu.VMEM((24, 384), F32),
            dma((6,)), dma((8,)), dma((8,)), dma((NZ,)), dma((NZ,)), dma((3, NZ)), dma((3, NZ)),
            dma((NZ,)), dma((NZ,)), dma((2, 2)), dma((2, 2)), dma((6,)), dma((6,)),
        ],
        compiler_params=pltpu.CompilerParams(
            collective_id=0, has_side_effects=True, vmem_limit_bytes=24 << 20
        ),
        name="exchange",
    )(*(pltpu.with_memory_space_constraint(v, pltpu.HBM) for v in (band_rows, tok, down, up, dg, ds)))


SPLIT = ((0, 1),)
ROWS = HALF * LEVELS


def patches(
    band_hbm, wd, wu, normed, ug, us, mix_hbm,
    out_hbm, band_ref, mix, fine, wu4, load_sem, store_sem,
):
    lat = lax.axis_index("lat")
    shift = jnp.minimum(lat, 1)
    loads = [
        pltpu.make_async_copy(mix_hbm, mix, load_sem.at[0]),
        pltpu.make_async_copy(band_hbm, band_ref, load_sem.at[1]),
    ]
    for load in loads:
        load.start()
    for g in range(4):
        wu4[g] = wu[:, C * g : C * (g + 1)]
    eps = 1e-05
    fine_gain, fine_shift = ug[...].reshape(1, C), us[...].reshape(1, C)
    rows_out = fine.reshape(MEMBERS, EXT, COLS, LEVELS, C)
    stores = []
    for members in SPLIT:
        def pick(g):
            return jnp.concatenate([normed[g, j, m] for j in range(4) for m in members], axis=0)

        coarse = None
        for g in range(4):
            term = jnp.dot(pick(g), wd[C * g : C * (g + 1), :], preferred_element_type=F32)
            coarse = term if coarse is None else coarse + term
        coarse = coarse.astype(BF)
        if members == SPLIT[0]:
            for load in loads:
                load.wait()
            bound = band_ref[0, 1] - band_ref[0, 0] + shift
        n = ROWS * len(members)
        for p in range(2):
            keep = 2 * lax.broadcasted_iota(jnp.int32, (HALF, LEVELS, C), 0) + p < bound
            for q in range(2):
                j0 = 1 - q
                grown = jnp.dot(coarse[n * j0 : n * (j0 + 3)], wu4[2 * p + q], preferred_element_type=F32)
                average = jnp.sum(grown, axis=1, keepdims=True) * (1.0 / C)
                grown = grown - average
                spread = jnp.sum(grown * grown, axis=1, keepdims=True) * (1.0 / C)
                unit = (grown * lax.rsqrt(spread + eps) * fine_gain + fine_shift).astype(BF)
                done = jnp.dot(unit, mix[...], preferred_element_type=F32).astype(BF)
                done = done.reshape(3, len(members), HALF, LEVELS, C)
                for j in range(3):
                    for i, m in enumerate(members):
                        fine[m, :, p, 2 * (j + j0) + q - 1] = jnp.where(keep, done[j, i], jnp.zeros_like(done[j, i]))
        for m in members:
            store = pltpu.make_async_copy(rows_out.at[m, pl.ds(shift, SLOTS)], out_hbm.at[m], store_sem.at[m])
            store.start()
            stores.append(store)
    for store in stores:
        store.wait()


def run_patches(band_rows, wd, wu, normed, ug, us, mix):
    vmem = pl.BlockSpec(memory_space=pltpu.VMEM)
    hbm = pl.BlockSpec(memory_space=pltpu.HBM)
    band_rows, mix = (pltpu.with_memory_space_constraint(v, pltpu.HBM) for v in (band_rows, mix))
    return pl.pallas_call(
        patches,
        out_shape=jax.ShapeDtypeStruct((MEMBERS, SLOTS, COLS, LEVELS, C), BF),
        in_specs=[hbm] + [vmem] * 5 + [hbm],
        out_specs=pl.BlockSpec(memory_space=pl.ANY),
        scratch_shapes=[
            pltpu.SMEM((1, 2), jnp.int32),
            pltpu.VMEM((C, C), BF),
            pltpu.VMEM((MEMBERS, HALF, 2, COLS, LEVELS, C), BF),
            pltpu.VMEM((4, 2 * C, C), BF),
            pltpu.SemaphoreType.DMA((2,)),
            pltpu.SemaphoreType.DMA((MEMBERS,)),
        ],
        compiler_params=pltpu.CompilerParams(vmem_limit_bytes=24 << 20),
        name="patches",
    )(band_rows, wd, wu, normed, ug, us, mix)


def body(
    tokens, band_rows, down_gain, down_shift, down_weight, up_weight, up_gain, up_shift, mix_weight
):
    tok = tokens.transpose(0, 2, 3, 1, 4)
    wd, wu, normed = run_exchange(band_rows, tok, down_weight, up_weight, down_gain, down_shift)
    out = run_patches(
        band_rows, wd.reshape(4 * C, 2 * C), wu.reshape(2 * C, 4 * C), normed, up_gain, up_shift, mix_weight
    )
    return out.transpose(0, 3, 1, 2, 4)


def solution(mesh):
    return jax.shard_map(
        body,
        mesh=mesh,
        in_specs=(
            P("mem", None, "lat", "lon", None),
            P("lat", None),
            P(),
            P(),
            P(("lon", "lat"), None),
            P(("lon", "lat"), None),
            P(),
            P(),
            P(),
        ),
        out_specs=P("mem", None, "lat", "lon", None),
        check_vma=False,
    )
```

```python
import functools

import jax
import jax.numpy as jnp
from jax import lax
from jax.experimental import pallas as pl
from jax.experimental.pallas import tpu as pltpu
from jax.sharding import PartitionSpec as P

MESH = pl.DeviceIdType.MESH
MEMBERS, LEVELS, SLOTS, COLS, C = 2, 8, 34, 6, 192
EXT = SLOTS + 2
HALF = EXT // 2
NZ = 8
ORDER = (1, 7, 2, 6, 3, 5, 4)
ARRIVE = (1, 7, 2, 6, 3, 5, 4)
LAG = 6
INSIDE = 0
COLS_AT = (-1, -1)
MIX = 0
BF = jnp.bfloat16
F32 = jnp.float32


def exchange(
    band_hbm, tok_hbm, down_hbm, up_hbm, dg_hbm, ds_hbm,
    wd, wu, normed,
    band_ref, dg, ds, tok, first_col, last_col, west, east, north, south, last, own_d, own_u, got_d, got_u, flat,
    load_sem, s1_send, s1_recv, z_send, z_recv, x_send, x_recv, pair_send, pair_recv,
    col_send, col_recv, row_send, row_recv,
):
    lon, lat, mem = lax.axis_index("lon"), lax.axis_index("lat"), lax.axis_index("mem")
    z, yh = lon // 2, lon % 2
    core, xx = lat % 2, lat // 2
    quarter = (xx + 2 * mem * MIX) % 4
    cy, ch = quarter % 2, quarter // 2
    shift = jnp.minimum(lat, 1)

    loads = [
        pltpu.make_async_copy(down_hbm, own_d, load_sem.at[0]),
        pltpu.make_async_copy(up_hbm, own_u, load_sem.at[1]),
        pltpu.make_async_copy(tok_hbm, tok.at[:, pl.ds(shift, SLOTS)], load_sem.at[2]),
        pltpu.make_async_copy(band_hbm, band_ref, load_sem.at[3]),
        pltpu.make_async_copy(dg_hbm, dg, load_sem.at[4]),
        pltpu.make_async_copy(ds_hbm, ds, load_sem.at[5]),
    ]
    for load in loads:
        load.start()

    @pl.when(lat > 0)
    def _():
        tok[:, 0] = jnp.zeros((MEMBERS, COLS, LEVELS, C), BF)
        tok[:, EXT - 1] = jnp.zeros((MEMBERS, COLS, LEVELS, C), BF)

    @pl.when(lat == 0)
    def _():
        tok[:, SLOTS:] = jnp.zeros((MEMBERS, 2, COLS, LEVELS, C), BF)

    lon_w, lon_e = (lon + 15) % 16, (lon + 1) % 16
    lat_n, lat_s = (lat + 7) % 8, (lat + 1) % 8
    lon_o, mem_o = 2 * z + 1 - yh, 1 - mem
    mate = (lon, lat + 1 - 2 * core, mem)

    def along(d):
        return (2 * ((z + d) % NZ) + yh, lat, mem)

    def across(s):
        return (lon, (lat + 2 * s) % 8, mem)

    barrier = pltpu.get_barrier_semaphore()
    partners = [(lon, (lat + d) % 8, mem) for d in range(1, 8)]
    partners += [(lon_o, (lat + d) % 8, mem_o) for d in range(8)]
    partners += [along(d) for d in range(1, NZ)]
    partners += [(lon, lat, mem_o)]
    partners += [
        (lon_w, lat, mem), (lon_e, lat, mem),
        (lon_w, lat_n, mem), (lon_w, lat_s, mem), (lon_e, lat_n, mem), (lon_e, lat_s, mem),
    ]
    for where in partners:
        pl.semaphore_signal(barrier, inc=1, device_id=where, device_id_type=MESH)
    loads[0].wait()
    loads[1].wait()
    pl.semaphore_wait(barrier, len(partners))

    def copy(src, dst, ssem, rsem, where):
        return pltpu.make_async_remote_copy(
            src_ref=src, dst_ref=dst, send_sem=ssem, recv_sem=rsem,
            device_id=where, device_id_type=MESH,
        )

    firsts = []

    def first(src, dst, i, slot, k, kind):
        lat_t = 2 * ((k + 2 * mem * MIX) % 4) + kind
        lat_f = 2 * ((k + 2 * mem_o * MIX) % 4) + kind
        firsts.append((lat_t != lat, copy(src, dst, s1_send.at[i], s1_recv.at[slot], (lon, lat_t, mem))))
        firsts.append((None, copy(src, dst, s1_send.at[i + 1], s1_recv.at[slot], (lon_o, lat_f, mem_o))))

    first(own_d, got_d.at[lat % 4], 0, lat % 4, yh + 2 * (lat // 4), 0)
    for h in range(2):
        first(own_u.at[:, 384 * h : 384 * (h + 1)], got_u.at[lat], 2 + 2 * h, lat, yh + 2 * h, 1)

    def each(op):
        for when, cp in firsts:
            if when is None:
                op(cp)
            else:
                @pl.when(when)
                def _():
                    op(cp)

    each(lambda cp: cp.start())

    for load in loads[2:]:
        load.wait()
    live = band_ref[0, 1] - band_ref[0, 0]
    last[...] = tok[:, pl.ds(jnp.clip(live - 1, 0, SLOTS - 1) + shift, 1)].reshape(MEMBERS, COLS, LEVELS, C)
    halves = tok.reshape(MEMBERS, HALF, 2, COLS, LEVELS, C)
    for m in range(MEMBERS):
        for i, box in ((0, first_col), (COLS - 1, last_col)):
            a, b = halves[m, :, 0, i], halves[m, :, 1, i]
            box[m, :, 0] = a[:, :, :128]
            box[m, :, 1] = b[:, :, :128]
            box[m, :, 2] = jnp.concatenate([a[:, :, 128:], b[:, :, 128:]], axis=2)

    cols = [
        [
            copy(first_col.at[m], east.at[m], col_send.at[m, 0], col_recv.at[m, 0], (lon_w, lat, mem)),
            copy(last_col.at[m], west.at[m], col_send.at[m, 1], col_recv.at[m, 1], (lon_e, lat, mem)),
        ]
        for m in range(MEMBERS)
    ]
    def start_cols(far):
        for m in range(MEMBERS):
            @pl.when(yh == far)
            def _():
                cols[m][1].start()

            @pl.when(yh != far)
            def _():
                cols[m][0].start()

    for far in range(2):
        if COLS_AT[far] == -2:
            start_cols(far)

    to_next = [
        copy(last, north.at[:, 1 : COLS + 1], row_send.at[0], row_recv.at[0], (lon, lat_s, mem)),
        copy(last.at[:, 0], north.at[:, COLS + 1], row_send.at[1], row_recv.at[1], (lon_w, lat_s, mem)),
        copy(last.at[:, COLS - 1], north.at[:, 0], row_send.at[2], row_recv.at[2], (lon_e, lat_s, mem)),
    ]
    to_prev = [
        copy(tok.at[:, shift], south.at[:, 1 : COLS + 1], row_send.at[3], row_recv.at[3], (lon, lat_n, mem)),
        copy(tok.at[:, shift, 0], south.at[:, COLS + 1], row_send.at[4], row_recv.at[4], (lon_w, lat_n, mem)),
        copy(tok.at[:, shift, COLS - 1], south.at[:, 0], row_send.at[5], row_recv.at[5], (lon_e, lat_n, mem)),
    ]

    @pl.when(lat < 7)
    def _():
        for cp in to_next:
            cp.start()

    @pl.when(lat > 0)
    def _():
        for cp in to_prev:
            cp.start()

    @pl.when(lat == 7)
    def _():
        south[...] = jnp.zeros_like(south)

    @pl.when(lat == 0)
    def _():
        north[...] = jnp.zeros_like(north)

    spot = (live + shift) // 2
    gains, shifts = dg[...].reshape(1, 4 * C), ds[...].reshape(1, 4 * C)

    def cell(m, j, q, p):
        i = 2 * j + q
        where = lax.broadcasted_iota(jnp.int32, (HALF, LEVELS, C), 0)
        if i in (0, COLS + 1):
            box = east if i else west
            x = jnp.concatenate([box[m, :, p], box[m, :, 2][:, :, 64 * p : 64 * p + 64]], axis=2)
            if p == 0:
                x = jnp.where(where + 1 == shift, north[m, i].reshape(1, LEVELS, C), x)
        else:
            x = tok.reshape(MEMBERS, HALF, 2, COLS, LEVELS, C)[m, :, p, i - 1]
        if p:
            x = jnp.where(where == spot, south[m, i].reshape(1, LEVELS, C), x)
        return x.reshape(HALF * LEVELS, C).astype(F32)

    def norm(j):
        @pl.loop(0, MEMBERS)
        def _(m):
            cells = {(q, p): cell(m, j, q, p) for q in range(2) for p in range(2)}
            total = sum(jnp.sum(x, axis=1, keepdims=True) for x in cells.values())
            average = total * (1.0 / (4 * C))
            cells = {key: x - average for key, x in cells.items()}
            total = sum(jnp.sum(x * x, axis=1, keepdims=True) for x in cells.values())
            scale = lax.rsqrt(total * (1.0 / (4 * C)) + 1e-05)
            done = []
            for (q, p), x in cells.items():
                g = 2 * q + p
                y = x * scale * gains[:, C * g : C * (g + 1)] + shifts[:, C * g : C * (g + 1)]
                done.append(y.astype(BF))
            normed[j, m] = jnp.concatenate(done, axis=1)

    def inside():
        @pl.when(lat < 7)
        def _():
            for cp in to_prev:
                cp.wait_recv()

        @pl.when(lat > 0)
        def _():
            for cp in to_next:
                cp.wait_recv()
            tok[:, 0] = north[:, 1 : COLS + 1]

        norm(1)
        norm(2)

    def border():
        for cp in cols[0] + cols[1]:
            cp.wait_recv()
        norm(0)
        norm(3)

    def centre(w):
        blocks = [w[:, :C], w[:, C:]]
        return jnp.concatenate([v - jnp.sum(v, axis=1, keepdims=True) * (1.0 / C) for v in blocks], axis=1)

    def gather(home, finish, parts, keep, got, flat, rows, full, mine):
        count = 24 // rows

        @pl.when(home)
        def _():
            keep()

        for i in range(count):
            @pl.when(jnp.logical_not(jnp.logical_and(home, lat % count == i)))
            def _():
                copy(parts, got.at[i], s1_send.at[0], s1_recv.at[i], mate).wait_recv()

        for i in range(count):
            flat[rows * i : rows * (i + 1), :] = got[i].astype(F32)
        mine(z)[...] = finish(flat[...]).astype(BF).reshape(1, 24, 384)
        z_out = [copy(mine(z), mine(z), z_send.at[d], z_recv.at[d], along(d)) for d in ORDER]
        for cp in z_out:
            cp.start()
        for far in range(2):
            if COLS_AT[far] == -1:
                start_cols(far)
        started = []

        def pass_on(b, t):
            part = mine(b)
            for s in range(2):
                cp = copy(part, part, x_send.at[s, t], x_recv.at[s, t], across(1 + 2 * s))
                cp.start()
                started.append(cp)
            side = b % 2
            cp = copy(part, part, x_send.at[2, t], x_recv.at[2, t], (lon + side * (lon_o - lon), lat, mem_o) if MIX else across(2))
            cp.start()
            started.append(cp)

        def hand_over(b, t):
            part = mine(b)
            for s in range(3):
                copy(part, part, x_send.at[s, t], x_recv.at[s, t], mate).wait_recv()
            whole = full.at[b]
            cp = copy(whole, whole, pair_send.at[t], pair_recv.at[t], mate)
            cp.start()
            started.append(cp)

        blocks = [(z + NZ - d) % NZ for d in (0,) + ARRIVE]
        for t, d in enumerate((0,) + ARRIVE):
            if d:
                copy(mine(z), mine(z), z_send.at[d], z_recv.at[d], mate).wait_recv()
            pass_on(blocks[t], t)
            for far in range(2):
                if COLS_AT[far] == t:
                    start_cols(far)
            if t == INSIDE:
                inside()
            if t >= LAG:
                hand_over(blocks[t - LAG], t - LAG)
        for t in range(NZ - LAG, NZ):
            hand_over(blocks[t], t)
        border()
        return z_out + started

    def take(other):
        for t, d in enumerate((0,) + ARRIVE):
            whole = other.at[(z + NZ - d) % NZ]
            copy(whole, whole, pair_send.at[t], pair_recv.at[t], mate).wait_recv()

    @pl.when(core == 0)
    def _():
        def keep():
            got_d[pl.ds(lat % 4, 1)] = own_d[...].reshape(1, 6, 384)

        def mine(b, n=1):
            return wd.at[pl.ds(b, n), pl.ds(pl.multiple_of(48 * cy + 24 * ch, 8), 24)]

        sent = gather(jnp.logical_and(yh == cy, lat // 4 == ch), lambda w: w, own_d, keep, got_d, flat, 6, wd, mine)
        take(wu)
        for cp in sent:
            cp.wait_send()

    @pl.when(core == 1)
    def _():
        def keep():
            got_u[pl.ds(lat, 1)] = own_u[:, pl.ds(pl.multiple_of(384 * ch, 128), 384)].reshape(1, 3, 384)

        def mine(b, n=1):
            return wu.at[pl.ds(b, n), pl.ds(pl.multiple_of(24 * cy, 8), 24), pl.ds(pl.multiple_of(384 * ch, 128), 384)]

        sent = gather(yh == cy, centre, own_u.at[:, :384], keep, got_u, flat, 3, wu, mine)
        take(wd)
        for cp in sent:
            cp.wait_send()

    each(lambda cp: cp.wait_send())
    for cp in cols[0] + cols[1]:
        cp.wait_send()

    @pl.when(lat < 7)
    def _():
        for cp in to_next:
            cp.wait_send()

    @pl.when(lat > 0)
    def _():
        for cp in to_prev:
            cp.wait_send()


def run_exchange(band_rows, tok, down, up, dg, ds):
    dma = pltpu.SemaphoreType.DMA
    vmem = pl.BlockSpec(memory_space=pltpu.VMEM)
    hbm = pl.BlockSpec(memory_space=pltpu.HBM)
    col = (MEMBERS, HALF, 3, LEVELS, 128)
    row = (MEMBERS, COLS + 2, LEVELS, C)
    return pl.pallas_call(
        exchange,
        out_shape=[
            jax.ShapeDtypeStruct((NZ, 96, 384), BF),
            jax.ShapeDtypeStruct((NZ, 48, 768), BF),
            jax.ShapeDtypeStruct((4, MEMBERS, HALF * LEVELS, 4 * C), BF),
        ],
        in_specs=[hbm] * 6,
        out_specs=[vmem] * 3,
        scratch_shapes=[
            pltpu.SMEM((1, 2), jnp.int32),
            pltpu.VMEM((4 * C,), F32),
            pltpu.VMEM((4 * C,), F32),
            pltpu.VMEM((MEMBERS, EXT, COLS, LEVELS, C), BF),
            pltpu.VMEM(col, BF),
            pltpu.VMEM(col, BF),
            pltpu.VMEM(col, BF),
            pltpu.VMEM(col, BF),
            pltpu.VMEM(row, BF),
            pltpu.VMEM(row, BF),
            pltpu.VMEM((MEMBERS, COLS, LEVELS, C), BF),
            pltpu.VMEM((6, 384), BF),
            pltpu.VMEM((3, 768), BF),
            pltpu.VMEM((4, 6, 384), BF),
            pltpu.VMEM((8, 3, 384), BF),
            pltpu.VMEM((24, 384), F32),
            dma((6,)), dma((8,)), dma((8,)), dma((NZ,)), dma((NZ,)), dma((3, NZ)), dma((3, NZ)),
            dma((NZ,)), dma((NZ,)), dma((2, 2)), dma((2, 2)), dma((6,)), dma((6,)),
        ],
        compiler_params=pltpu.CompilerParams(
            collective_id=0, has_side_effects=True, vmem_limit_bytes=24 << 20
        ),
        name="exchange",
    )(*(pltpu.with_memory_space_constraint(v, pltpu.HBM) for v in (band_rows, tok, down, up, dg, ds)))


SPLIT = ((0, 1),)
ROWS = HALF * LEVELS


def patches(
    band_hbm, wd, wu, normed, ug, us, mix_hbm,
    out_hbm, band_ref, mix, fine, wu4, load_sem, store_sem,
):
    lat = lax.axis_index("lat")
    shift = jnp.minimum(lat, 1)
    loads = [
        pltpu.make_async_copy(mix_hbm, mix, load_sem.at[0]),
        pltpu.make_async_copy(band_hbm, band_ref, load_sem.at[1]),
    ]
    for load in loads:
        load.start()
    for g in range(4):
        wu4[g] = wu[:, C * g : C * (g + 1)]
    eps = 1e-05
    fine_gain, fine_shift = ug[...].reshape(1, C), us[...].reshape(1, C)
    pairs = out_hbm.reshape(MEMBERS, SLOTS // 2, 2, COLS, LEVELS, C)
    stores = []
    for members in SPLIT:
        def pick():
            return jnp.concatenate([normed[j, m] for j in range(4) for m in members], axis=0)

        coarse = jnp.dot(pick(), wd[...], preferred_element_type=F32).astype(BF)
        if members == SPLIT[0]:
            for load in loads:
                load.wait()
            bound = band_ref[0, 1] - band_ref[0, 0] + shift
        n = ROWS * len(members)
        for p in range(2):
            keep = 2 * lax.broadcasted_iota(jnp.int32, (HALF, LEVELS, C), 0) + p < bound
            for q in range(2):
                j0 = 1 - q
                grown = jnp.dot(coarse[n * j0 : n * (j0 + 3)], wu4[2 * p + q], preferred_element_type=F32)
                spread = jnp.sum(grown * grown, axis=1, keepdims=True) * (1.0 / C)
                unit = (grown * lax.rsqrt(spread + eps) * fine_gain + fine_shift).astype(BF)
                done = jnp.dot(unit, mix[...], preferred_element_type=F32).astype(BF)
                done = done.reshape(3, len(members), HALF, LEVELS, C)
                for j in range(3):
                    for i, m in enumerate(members):
                        fine[m, :, p, 2 * (j + j0) + q - 1] = jnp.where(keep, done[j, i], jnp.zeros_like(done[j, i]))
            for m in members:
                store = pltpu.make_async_copy(
                    fine.at[m, pl.ds(shift * (1 - p), SLOTS // 2), p],
                    pairs.at[m, :, p + shift - 2 * p * shift],
                    store_sem.at[m, p],
                )
                store.start()
                stores.append(store)
    for store in stores:
        store.wait()


def run_patches(band_rows, wd, wu, normed, ug, us, mix):
    vmem = pl.BlockSpec(memory_space=pltpu.VMEM)
    hbm = pl.BlockSpec(memory_space=pltpu.HBM)
    band_rows, mix = (pltpu.with_memory_space_constraint(v, pltpu.HBM) for v in (band_rows, mix))
    return pl.pallas_call(
        patches,
        out_shape=jax.ShapeDtypeStruct((MEMBERS, SLOTS, COLS, LEVELS, C), BF),
        in_specs=[hbm] + [vmem] * 5 + [hbm],
        out_specs=pl.BlockSpec(memory_space=pl.ANY),
        scratch_shapes=[
            pltpu.SMEM((1, 2), jnp.int32),
            pltpu.VMEM((C, C), BF),
            pltpu.VMEM((MEMBERS, HALF, 2, COLS, LEVELS, C), BF),
            pltpu.VMEM((4, 2 * C, C), BF),
            pltpu.SemaphoreType.DMA((2,)),
            pltpu.SemaphoreType.DMA((MEMBERS, 2)),
        ],
        compiler_params=pltpu.CompilerParams(vmem_limit_bytes=24 << 20),
        name="patches",
    )(band_rows, wd, wu, normed, ug, us, mix)


def body(
    tokens, band_rows, down_gain, down_shift, down_weight, up_weight, up_gain, up_shift, mix_weight
):
    tok = tokens.transpose(0, 2, 3, 1, 4)
    wd, wu, normed = run_exchange(band_rows, tok, down_weight, up_weight, down_gain, down_shift)
    out = run_patches(
        band_rows, wd.reshape(4 * C, 2 * C), wu.reshape(2 * C, 4 * C), normed, up_gain, up_shift, mix_weight
    )
    return out.transpose(0, 3, 1, 2, 4)


def solution(mesh):
    return jax.shard_map(
        body,
        mesh=mesh,
        in_specs=(
            P("mem", None, "lat", "lon", None),
            P("lat", None),
            P(),
            P(),
            P(("lon", "lat"), None),
            P(("lon", "lat"), None),
            P(),
            P(),
            P(),
        ),
        out_specs=P("mem", None, "lat", "lon", None),
        check_vma=False,
    )
```

```python
import functools

import jax
import jax.numpy as jnp
from jax import lax
from jax.experimental import pallas as pl
from jax.experimental.pallas import tpu as pltpu
from jax.sharding import PartitionSpec as P

MESH = pl.DeviceIdType.MESH
MEMBERS, LEVELS, SLOTS, COLS, C = 2, 8, 34, 6, 192
EXT = SLOTS + 2
HALF = EXT // 2
NZ = 8
ORDER = (1, 7, 2, 6, 3, 5, 4)
ARRIVE = (1, 7, 2, 6, 3, 5, 4)
LAG = 6
BORDER_AT = (7, 8)
INSIDE = 0
COLS_AT = (-1, -1)
MIX = 0
BF = jnp.bfloat16
F32 = jnp.float32


def exchange(
    band_hbm, tok_hbm, down_hbm, up_hbm, dg_hbm, ds_hbm,
    wd, wu, normed,
    band_ref, dg, ds, tok, first_col, last_col, west, east, north, south, last, own_d, own_u, got_d, got_u, flat,
    load_sem, s1_send, s1_recv, z_send, z_recv, x_send, x_recv, pair_send, pair_recv,
    col_send, col_recv, row_send, row_recv,
):
    lon, lat, mem = lax.axis_index("lon"), lax.axis_index("lat"), lax.axis_index("mem")
    z, yh = lon // 2, lon % 2
    core, xx = lat % 2, lat // 2
    quarter = (xx + 2 * mem * MIX) % 4
    cy, ch = quarter % 2, quarter // 2
    shift = jnp.minimum(lat, 1)

    loads = [
        pltpu.make_async_copy(down_hbm, own_d, load_sem.at[0]),
        pltpu.make_async_copy(up_hbm, own_u, load_sem.at[1]),
        pltpu.make_async_copy(tok_hbm, tok.at[:, pl.ds(shift, SLOTS)], load_sem.at[2]),
        pltpu.make_async_copy(band_hbm, band_ref, load_sem.at[3]),
        pltpu.make_async_copy(dg_hbm, dg, load_sem.at[4]),
        pltpu.make_async_copy(ds_hbm, ds, load_sem.at[5]),
    ]
    for load in loads:
        load.start()

    @pl.when(lat > 0)
    def _():
        tok[:, 0] = jnp.zeros((MEMBERS, COLS, LEVELS, C), BF)
        tok[:, EXT - 1] = jnp.zeros((MEMBERS, COLS, LEVELS, C), BF)

    @pl.when(lat == 0)
    def _():
        tok[:, SLOTS:] = jnp.zeros((MEMBERS, 2, COLS, LEVELS, C), BF)

    lon_w, lon_e = (lon + 15) % 16, (lon + 1) % 16
    lat_n, lat_s = (lat + 7) % 8, (lat + 1) % 8
    lon_o, mem_o = 2 * z + 1 - yh, 1 - mem
    mate = (lon, lat + 1 - 2 * core, mem)

    def along(d):
        return (2 * ((z + d) % NZ) + yh, lat, mem)

    def across(s):
        return (lon, (lat + 2 * s) % 8, mem)

    barrier = pltpu.get_barrier_semaphore()
    partners = [(lon, (lat + d) % 8, mem) for d in range(1, 8)]
    partners += [(lon_o, (lat + d) % 8, mem_o) for d in range(8)]
    partners += [along(d) for d in range(1, NZ)]
    partners += [(lon, lat, mem_o)]
    partners += [
        (lon_w, lat, mem), (lon_e, lat, mem),
        (lon_w, lat_n, mem), (lon_w, lat_s, mem), (lon_e, lat_n, mem), (lon_e, lat_s, mem),
    ]
    for where in partners:
        pl.semaphore_signal(barrier, inc=1, device_id=where, device_id_type=MESH)
    loads[0].wait()
    loads[1].wait()
    pl.semaphore_wait(barrier, len(partners))

    def copy(src, dst, ssem, rsem, where):
        return pltpu.make_async_remote_copy(
            src_ref=src, dst_ref=dst, send_sem=ssem, recv_sem=rsem,
            device_id=where, device_id_type=MESH,
        )

    firsts = []

    def first(src, dst, i, slot, k, kind):
        lat_t = 2 * ((k + 2 * mem * MIX) % 4) + kind
        lat_f = 2 * ((k + 2 * mem_o * MIX) % 4) + kind
        firsts.append((lat_t != lat, copy(src, dst, s1_send.at[i], s1_recv.at[slot], (lon, lat_t, mem))))
        firsts.append((None, copy(src, dst, s1_send.at[i + 1], s1_recv.at[slot], (lon_o, lat_f, mem_o))))

    first(own_d, got_d.at[lat % 4], 0, lat % 4, yh + 2 * (lat // 4), 0)
    for h in range(2):
        first(own_u.at[:, 384 * h : 384 * (h + 1)], got_u.at[lat], 2 + 2 * h, lat, yh + 2 * h, 1)

    def each(op):
        for when, cp in firsts:
            if when is None:
                op(cp)
            else:
                @pl.when(when)
                def _():
                    op(cp)

    each(lambda cp: cp.start())

    for load in loads[2:]:
        load.wait()
    live = band_ref[0, 1] - band_ref[0, 0]
    last[...] = tok[:, pl.ds(jnp.clip(live - 1, 0, SLOTS - 1) + shift, 1)].reshape(MEMBERS, COLS, LEVELS, C)
    halves = tok.reshape(MEMBERS, HALF, 2, COLS, LEVELS, C)
    for m in range(MEMBERS):
        for i, box in ((0, first_col), (COLS - 1, last_col)):
            a, b = halves[m, :, 0, i], halves[m, :, 1, i]
            box[m, :, 0] = a[:, :, :128]
            box[m, :, 1] = b[:, :, :128]
            box[m, :, 2] = jnp.concatenate([a[:, :, 128:], b[:, :, 128:]], axis=2)

    cols = [
        [
            copy(first_col.at[m], east.at[m], col_send.at[m, 0], col_recv.at[m, 0], (lon_w, lat, mem)),
            copy(last_col.at[m], west.at[m], col_send.at[m, 1], col_recv.at[m, 1], (lon_e, lat, mem)),
        ]
        for m in range(MEMBERS)
    ]
    def start_cols(far):
        for m in range(MEMBERS):
            @pl.when(yh == far)
            def _():
                cols[m][1].start()

            @pl.when(yh != far)
            def _():
                cols[m][0].start()

    for far in range(2):
        if COLS_AT[far] == -2:
            start_cols(far)

    to_next = [
        copy(last, north.at[:, 1 : COLS + 1], row_send.at[0], row_recv.at[0], (lon, lat_s, mem)),
        copy(last.at[:, 0], north.at[:, COLS + 1], row_send.at[1], row_recv.at[1], (lon_w, lat_s, mem)),
        copy(last.at[:, COLS - 1], north.at[:, 0], row_send.at[2], row_recv.at[2], (lon_e, lat_s, mem)),
    ]
    to_prev = [
        copy(tok.at[:, shift], south.at[:, 1 : COLS + 1], row_send.at[3], row_recv.at[3], (lon, lat_n, mem)),
        copy(tok.at[:, shift, 0], south.at[:, COLS + 1], row_send.at[4], row_recv.at[4], (lon_w, lat_n, mem)),
        copy(tok.at[:, shift, COLS - 1], south.at[:, 0], row_send.at[5], row_recv.at[5], (lon_e, lat_n, mem)),
    ]

    @pl.when(lat < 7)
    def _():
        for cp in to_next:
            cp.start()

    @pl.when(lat > 0)
    def _():
        for cp in to_prev:
            cp.start()

    @pl.when(lat == 7)
    def _():
        south[...] = jnp.zeros_like(south)

    @pl.when(lat == 0)
    def _():
        north[...] = jnp.zeros_like(north)

    spot = (live + shift) // 2
    gains, shifts = dg[...].reshape(1, 4 * C), ds[...].reshape(1, 4 * C)

    def cell(m, j, q, p):
        i = 2 * j + q
        where = lax.broadcasted_iota(jnp.int32, (HALF, LEVELS, C), 0)
        if i in (0, COLS + 1):
            box = east if i else west
            x = jnp.concatenate([box[m, :, p], box[m, :, 2][:, :, 64 * p : 64 * p + 64]], axis=2)
            if p == 0:
                x = jnp.where(where + 1 == shift, north[m, i].reshape(1, LEVELS, C), x)
        else:
            x = tok.reshape(MEMBERS, HALF, 2, COLS, LEVELS, C)[m, :, p, i - 1]
        if p:
            x = jnp.where(where == spot, south[m, i].reshape(1, LEVELS, C), x)
        return x.reshape(HALF * LEVELS, C).astype(F32)

    def norm(js, m):
        keys = [(j, q, p) for j in js for q in range(2) for p in range(2)]
        cells = {key: cell(m, *key) for key in keys}
        average, scale = {}, {}
        for j in js:
            total = sum(jnp.sum(cells[key], axis=1, keepdims=True) for key in keys if key[0] == j)
            average[j] = total * (1.0 / (4 * C))
        cells = {key: x - average[key[0]] for key, x in cells.items()}
        for j in js:
            total = sum(jnp.sum(cells[key] * cells[key], axis=1, keepdims=True) for key in keys if key[0] == j)
            scale[j] = lax.rsqrt(total * (1.0 / (4 * C)) + 1e-05)
        for j in js:
            done = []
            for q in range(2):
                for p in range(2):
                    g = 2 * q + p
                    y = cells[j, q, p] * scale[j] * gains[:, C * g : C * (g + 1)] + shifts[:, C * g : C * (g + 1)]
                    done.append(y.astype(BF))
            normed[j, m] = jnp.concatenate(done, axis=1)

    def inside():
        @pl.when(lat < 7)
        def _():
            for cp in to_prev:
                cp.wait_recv()

        @pl.when(lat > 0)
        def _():
            for cp in to_next:
                cp.wait_recv()
            tok[:, 0] = north[:, 1 : COLS + 1]

        for m in range(MEMBERS):
            norm((1, 2), m)

    def border(m):
        for cp in cols[m]:
            cp.wait_recv()
        norm((0, COLS // 2), m)

    def centre(w):
        blocks = [w[:, :C], w[:, C:]]
        return jnp.concatenate([v - jnp.sum(v, axis=1, keepdims=True) * (1.0 / C) for v in blocks], axis=1)

    def gather(home, finish, parts, keep, got, flat, rows, full, mine):
        count = 24 // rows

        @pl.when(home)
        def _():
            keep()

        for i in range(count):
            @pl.when(jnp.logical_not(jnp.logical_and(home, lat % count == i)))
            def _():
                copy(parts, got.at[i], s1_send.at[0], s1_recv.at[i], mate).wait_recv()

        for i in range(count):
            flat[rows * i : rows * (i + 1), :] = got[i].astype(F32)
        mine(z)[...] = finish(flat[...]).astype(BF).reshape(1, 24, 384)
        z_out = [copy(mine(z), mine(z), z_send.at[d], z_recv.at[d], along(d)) for d in ORDER]
        for cp in z_out:
            cp.start()
        for far in range(2):
            if COLS_AT[far] == -1:
                start_cols(far)
        started = []

        def pass_on(b, t):
            part = mine(b)
            for s in range(2):
                cp = copy(part, part, x_send.at[s, t], x_recv.at[s, t], across(1 + 2 * s))
                cp.start()
                started.append(cp)
            side = b % 2
            cp = copy(part, part, x_send.at[2, t], x_recv.at[2, t], (lon + side * (lon_o - lon), lat, mem_o) if MIX else across(2))
            cp.start()
            started.append(cp)

        def hand_over(b, t):
            for m in range(MEMBERS):
                if t == BORDER_AT[m]:
                    border(m)
            part = mine(b)
            for s in range(3):
                copy(part, part, x_send.at[s, t], x_recv.at[s, t], mate).wait_recv()
            whole = full.at[b]
            cp = copy(whole, whole, pair_send.at[t], pair_recv.at[t], mate)
            cp.start()
            started.append(cp)

        blocks = [(z + NZ - d) % NZ for d in (0,) + ARRIVE]
        for t, d in enumerate((0,) + ARRIVE):
            if d:
                copy(mine(z), mine(z), z_send.at[d], z_recv.at[d], mate).wait_recv()
            pass_on(blocks[t], t)
            for far in range(2):
                if COLS_AT[far] == t:
                    start_cols(far)
            if t == INSIDE:
                inside()
            if t >= LAG:
                hand_over(blocks[t - LAG], t - LAG)
        for t in range(NZ - LAG, NZ):
            hand_over(blocks[t], t)
        for m in range(MEMBERS):
            if BORDER_AT[m] == NZ:
                border(m)
        return z_out + started

    def take(other):
        for t, d in enumerate((0,) + ARRIVE):
            whole = other.at[(z + NZ - d) % NZ]
            copy(whole, whole, pair_send.at[t], pair_recv.at[t], mate).wait_recv()

    @pl.when(core == 0)
    def _():
        def keep():
            got_d[pl.ds(lat % 4, 1)] = own_d[...].reshape(1, 6, 384)

        def mine(b, n=1):
            return wd.at[pl.ds(b, n), pl.ds(pl.multiple_of(48 * cy + 24 * ch, 8), 24)]

        sent = gather(jnp.logical_and(yh == cy, lat // 4 == ch), lambda w: w, own_d, keep, got_d, flat, 6, wd, mine)
        take(wu)
        for cp in sent:
            cp.wait_send()

    @pl.when(core == 1)
    def _():
        def keep():
            got_u[pl.ds(lat, 1)] = own_u[:, pl.ds(pl.multiple_of(384 * ch, 128), 384)].reshape(1, 3, 384)

        def mine(b, n=1):
            return wu.at[pl.ds(b, n), pl.ds(pl.multiple_of(24 * cy, 8), 24), pl.ds(pl.multiple_of(384 * ch, 128), 384)]

        sent = gather(yh == cy, centre, own_u.at[:, :384], keep, got_u, flat, 3, wu, mine)
        take(wd)
        for cp in sent:
            cp.wait_send()

    each(lambda cp: cp.wait_send())
    for cp in cols[0] + cols[1]:
        cp.wait_send()

    @pl.when(lat < 7)
    def _():
        for cp in to_next:
            cp.wait_send()

    @pl.when(lat > 0)
    def _():
        for cp in to_prev:
            cp.wait_send()


def run_exchange(band_rows, tok, down, up, dg, ds):
    dma = pltpu.SemaphoreType.DMA
    vmem = pl.BlockSpec(memory_space=pltpu.VMEM)
    hbm = pl.BlockSpec(memory_space=pltpu.HBM)
    col = (MEMBERS, HALF, 3, LEVELS, 128)
    row = (MEMBERS, COLS + 2, LEVELS, C)
    return pl.pallas_call(
        exchange,
        out_shape=[
            jax.ShapeDtypeStruct((NZ, 96, 384), BF),
            jax.ShapeDtypeStruct((NZ, 48, 768), BF),
            jax.ShapeDtypeStruct((4, MEMBERS, HALF * LEVELS, 4 * C), BF),
        ],
        in_specs=[hbm] * 6,
        out_specs=[vmem] * 3,
        scratch_shapes=[
            pltpu.SMEM((1, 2), jnp.int32),
            pltpu.VMEM((4 * C,), F32),
            pltpu.VMEM((4 * C,), F32),
            pltpu.VMEM((MEMBERS, EXT, COLS, LEVELS, C), BF),
            pltpu.VMEM(col, BF),
            pltpu.VMEM(col, BF),
            pltpu.VMEM(col, BF),
            pltpu.VMEM(col, BF),
            pltpu.VMEM(row, BF),
            pltpu.VMEM(row, BF),
            pltpu.VMEM((MEMBERS, COLS, LEVELS, C), BF),
            pltpu.VMEM((6, 384), BF),
            pltpu.VMEM((3, 768), BF),
            pltpu.VMEM((4, 6, 384), BF),
            pltpu.VMEM((8, 3, 384), BF),
            pltpu.VMEM((24, 384), F32),
            dma((6,)), dma((8,)), dma((8,)), dma((NZ,)), dma((NZ,)), dma((3, NZ)), dma((3, NZ)),
            dma((NZ,)), dma((NZ,)), dma((2, 2)), dma((2, 2)), dma((6,)), dma((6,)),
        ],
        compiler_params=pltpu.CompilerParams(
            collective_id=0, has_side_effects=True, vmem_limit_bytes=24 << 20
        ),
        name="exchange",
    )(*(pltpu.with_memory_space_constraint(v, pltpu.HBM) for v in (band_rows, tok, down, up, dg, ds)))


SPLIT = ((0, 1),)
ROWS = HALF * LEVELS


def patches(
    band_hbm, wd, wu, normed, ug, us, mix_hbm,
    out_hbm, band_ref, mix, fine, wu4, load_sem, store_sem,
):
    lat = lax.axis_index("lat")
    shift = jnp.minimum(lat, 1)
    loads = [
        pltpu.make_async_copy(mix_hbm, mix, load_sem.at[0]),
        pltpu.make_async_copy(band_hbm, band_ref, load_sem.at[1]),
    ]
    for load in loads:
        load.start()
    for g in range(4):
        wu4[g] = wu[:, C * g : C * (g + 1)]
    eps = 1e-05
    fine_gain, fine_shift = ug[...].reshape(1, C), us[...].reshape(1, C)
    pairs = out_hbm.reshape(MEMBERS, SLOTS // 2, 2, COLS, LEVELS, C)
    stores = []
    for members in SPLIT:
        def pick():
            return jnp.concatenate([normed[j, m] for j in range(4) for m in members], axis=0)

        coarse = jnp.dot(pick(), wd[...], preferred_element_type=F32).astype(BF)
        if members == SPLIT[0]:
            for load in loads:
                load.wait()
            bound = band_ref[0, 1] - band_ref[0, 0] + shift
        n = ROWS * len(members)
        for p in range(2):
            keep = 2 * lax.broadcasted_iota(jnp.int32, (HALF, LEVELS, C), 0) + p < bound
            for q in range(2):
                j0 = 1 - q
                grown = jnp.dot(coarse[n * j0 : n * (j0 + 3)], wu4[2 * p + q], preferred_element_type=F32)
                spread = jnp.sum(grown * grown, axis=1, keepdims=True) * (1.0 / C)
                unit = (grown * lax.rsqrt(spread + eps) * fine_gain + fine_shift).astype(BF)
                done = jnp.dot(unit, mix[...], preferred_element_type=F32).astype(BF)
                done = done.reshape(3, len(members), HALF, LEVELS, C)
                for j in range(3):
                    for i, m in enumerate(members):
                        fine[m, :, p, 2 * (j + j0) + q - 1] = jnp.where(keep, done[j, i], jnp.zeros_like(done[j, i]))
            for m in members:
                store = pltpu.make_async_copy(
                    fine.at[m, pl.ds(shift * (1 - p), SLOTS // 2), p],
                    pairs.at[m, :, p + shift - 2 * p * shift],
                    store_sem.at[m, p],
                )
                store.start()
                stores.append(store)
    for store in stores:
        store.wait()


def run_patches(band_rows, wd, wu, normed, ug, us, mix):
    vmem = pl.BlockSpec(memory_space=pltpu.VMEM)
    hbm = pl.BlockSpec(memory_space=pltpu.HBM)
    band_rows, mix = (pltpu.with_memory_space_constraint(v, pltpu.HBM) for v in (band_rows, mix))
    return pl.pallas_call(
        patches,
        out_shape=jax.ShapeDtypeStruct((MEMBERS, SLOTS, COLS, LEVELS, C), BF),
        in_specs=[hbm] + [vmem] * 5 + [hbm],
        out_specs=pl.BlockSpec(memory_space=pl.ANY),
        scratch_shapes=[
            pltpu.SMEM((1, 2), jnp.int32),
            pltpu.VMEM((C, C), BF),
            pltpu.VMEM((MEMBERS, HALF, 2, COLS, LEVELS, C), BF),
            pltpu.VMEM((4, 2 * C, C), BF),
            pltpu.SemaphoreType.DMA((2,)),
            pltpu.SemaphoreType.DMA((MEMBERS, 2)),
        ],
        compiler_params=pltpu.CompilerParams(vmem_limit_bytes=24 << 20),
        name="patches",
    )(band_rows, wd, wu, normed, ug, us, mix)


def body(
    tokens, band_rows, down_gain, down_shift, down_weight, up_weight, up_gain, up_shift, mix_weight
):
    tok = tokens.transpose(0, 2, 3, 1, 4)
    wd, wu, normed = run_exchange(band_rows, tok, down_weight, up_weight, down_gain, down_shift)
    out = run_patches(
        band_rows, wd.reshape(4 * C, 2 * C), wu.reshape(2 * C, 4 * C), normed, up_gain, up_shift, mix_weight
    )
    return out.transpose(0, 3, 1, 2, 4)


def solution(mesh):
    return jax.shard_map(
        body,
        mesh=mesh,
        in_specs=(
            P("mem", None, "lat", "lon", None),
            P("lat", None),
            P(),
            P(),
            P(("lon", "lat"), None),
            P(("lon", "lat"), None),
            P(),
            P(),
            P(),
        ),
        out_specs=P("mem", None, "lat", "lon", None),
        check_vma=False,
    )
```

```python
import functools

import jax
import jax.numpy as jnp
from jax import lax
from jax.experimental import pallas as pl
from jax.experimental.pallas import tpu as pltpu
from jax.sharding import PartitionSpec as P

MESH = pl.DeviceIdType.MESH
MEMBERS, LEVELS, SLOTS, COLS, C = 2, 8, 34, 6, 192
EXT = SLOTS + 2
HALF = EXT // 2
NZ = 8
ORDER = (1, 7, 2, 6, 3, 5, 4)
ARRIVE = (1, 7, 2, 6, 3, 5, 4)
LAG = 6
BORDER_AT = (7, 8)
INSIDE = 0
COLS_AT = (-1, -1)
MIX = 0
BF = jnp.bfloat16
F32 = jnp.float32


def exchange(
    band_hbm, tok_hbm, down_hbm, up_hbm, dg_hbm, ds_hbm,
    wd, wu, normed,
    band_ref, dg, ds, tok, first_col, last_col, west, east, north, south, last, own_d, own_u, got_d, got_u, flat,
    load_sem, s1_send, s1_recv, z_send, z_recv, x_send, x_recv, pair_send, pair_recv,
    col_send, col_recv, row_send, row_recv,
):
    lon, lat, mem = lax.axis_index("lon"), lax.axis_index("lat"), lax.axis_index("mem")
    z, yh = lon // 2, lon % 2
    core, xx = lat % 2, lat // 2
    quarter = (xx + 2 * mem * MIX) % 4
    cy, ch = quarter % 2, quarter // 2
    shift = jnp.minimum(lat, 1)

    loads = [
        pltpu.make_async_copy(down_hbm, own_d, load_sem.at[0]),
        pltpu.make_async_copy(up_hbm, own_u, load_sem.at[1]),
        pltpu.make_async_copy(tok_hbm, tok.at[:, pl.ds(shift, SLOTS)], load_sem.at[2]),
        pltpu.make_async_copy(band_hbm, band_ref, load_sem.at[3]),
        pltpu.make_async_copy(dg_hbm, dg, load_sem.at[4]),
        pltpu.make_async_copy(ds_hbm, ds, load_sem.at[5]),
    ]
    for load in loads:
        load.start()

    @pl.when(lat > 0)
    def _():
        tok[:, 0] = jnp.zeros((MEMBERS, COLS, LEVELS, C), BF)
        tok[:, EXT - 1] = jnp.zeros((MEMBERS, COLS, LEVELS, C), BF)

    @pl.when(lat == 0)
    def _():
        tok[:, SLOTS:] = jnp.zeros((MEMBERS, 2, COLS, LEVELS, C), BF)

    lon_w, lon_e = (lon + 15) % 16, (lon + 1) % 16
    lat_n, lat_s = (lat + 7) % 8, (lat + 1) % 8
    lon_o, mem_o = 2 * z + 1 - yh, 1 - mem
    mate = (lon, lat + 1 - 2 * core, mem)

    def along(d):
        return (2 * ((z + d) % NZ) + yh, lat, mem)

    def across(s):
        return (lon, (lat + 2 * s) % 8, mem)

    barrier = pltpu.get_barrier_semaphore()
    partners = [(lon, (lat + d) % 8, mem) for d in range(1, 8)]
    partners += [(lon_o, (lat + d) % 8, mem_o) for d in range(8)]
    partners += [along(d) for d in range(1, NZ)]
    partners += [(lon, lat, mem_o)]
    partners += [
        (lon_w, lat, mem), (lon_e, lat, mem),
        (lon_w, lat_n, mem), (lon_w, lat_s, mem), (lon_e, lat_n, mem), (lon_e, lat_s, mem),
    ]
    for where in partners:
        pl.semaphore_signal(barrier, inc=1, device_id=where, device_id_type=MESH)
    loads[0].wait()
    loads[1].wait()
    pl.semaphore_wait(barrier, len(partners))

    def copy(src, dst, ssem, rsem, where):
        return pltpu.make_async_remote_copy(
            src_ref=src, dst_ref=dst, send_sem=ssem, recv_sem=rsem,
            device_id=where, device_id_type=MESH,
        )

    firsts = []

    def first(src, dst, i, slot, k, kind):
        lat_t = 2 * ((k + 2 * mem * MIX) % 4) + kind
        lat_f = 2 * ((k + 2 * mem_o * MIX) % 4) + kind
        firsts.append((lat_t != lat, copy(src, dst, s1_send.at[i], s1_recv.at[slot], (lon, lat_t, mem))))
        firsts.append((None, copy(src, dst, s1_send.at[i + 1], s1_recv.at[slot], (lon_o, lat_f, mem_o))))

    first(own_d, got_d.at[lat % 4], 0, lat % 4, yh + 2 * (lat // 4), 0)
    for h in range(2):
        first(own_u.at[:, 384 * h : 384 * (h + 1)], got_u.at[lat], 2 + 2 * h, lat, yh + 2 * h, 1)

    def each(op):
        for when, cp in firsts:
            if when is None:
                op(cp)
            else:
                @pl.when(when)
                def _():
                    op(cp)

    each(lambda cp: cp.start())

    for load in loads[2:]:
        load.wait()
    live = band_ref[0, 1] - band_ref[0, 0]
    last[...] = tok[:, pl.ds(jnp.clip(live - 1, 0, SLOTS - 1) + shift, 1)].reshape(MEMBERS, COLS, LEVELS, C)
    halves = tok.reshape(MEMBERS, HALF, 2, COLS, LEVELS, C)
    for m in range(MEMBERS):
        for i, box in ((0, first_col), (COLS - 1, last_col)):
            a, b = halves[m, :, 0, i], halves[m, :, 1, i]
            box[m, :, 0] = a[:, :, :128]
            box[m, :, 1] = b[:, :, :128]
            box[m, :, 2] = jnp.concatenate([a[:, :, 128:], b[:, :, 128:]], axis=2)

    cols = [
        [
            copy(first_col.at[m], east.at[m], col_send.at[m, 0], col_recv.at[m, 0], (lon_w, lat, mem)),
            copy(last_col.at[m], west.at[m], col_send.at[m, 1], col_recv.at[m, 1], (lon_e, lat, mem)),
        ]
        for m in range(MEMBERS)
    ]
    def start_cols(far):
        for m in range(MEMBERS):
            @pl.when(yh == far)
            def _():
                cols[m][1].start()

            @pl.when(yh != far)
            def _():
                cols[m][0].start()

    for far in range(2):
        if COLS_AT[far] == -2:
            start_cols(far)

    to_next = [
        copy(last, north.at[:, 1 : COLS + 1], row_send.at[0], row_recv.at[0], (lon, lat_s, mem)),
        copy(last.at[:, 0], north.at[:, COLS + 1], row_send.at[1], row_recv.at[1], (lon_w, lat_s, mem)),
        copy(last.at[:, COLS - 1], north.at[:, 0], row_send.at[2], row_recv.at[2], (lon_e, lat_s, mem)),
    ]
    to_prev = [
        copy(tok.at[:, shift], south.at[:, 1 : COLS + 1], row_send.at[3], row_recv.at[3], (lon, lat_n, mem)),
        copy(tok.at[:, shift, 0], south.at[:, COLS + 1], row_send.at[4], row_recv.at[4], (lon_w, lat_n, mem)),
        copy(tok.at[:, shift, COLS - 1], south.at[:, 0], row_send.at[5], row_recv.at[5], (lon_e, lat_n, mem)),
    ]

    @pl.when(lat < 7)
    def _():
        for cp in to_next:
            cp.start()

    @pl.when(lat > 0)
    def _():
        for cp in to_prev:
            cp.start()

    @pl.when(lat == 7)
    def _():
        south[...] = jnp.zeros_like(south)

    @pl.when(lat == 0)
    def _():
        north[...] = jnp.zeros_like(north)

    spot = (live + shift) // 2
    gains, shifts = dg[...].reshape(1, 4 * C), ds[...].reshape(1, 4 * C)

    def cell(m, j, q, p):
        i = 2 * j + q
        where = lax.broadcasted_iota(jnp.int32, (HALF, LEVELS, C), 0)
        if i in (0, COLS + 1):
            box = east if i else west
            x = jnp.concatenate([box[m, :, p], box[m, :, 2][:, :, 64 * p : 64 * p + 64]], axis=2)
            if p == 0:
                x = jnp.where(where + 1 == shift, north[m, i].reshape(1, LEVELS, C), x)
        else:
            x = tok.reshape(MEMBERS, HALF, 2, COLS, LEVELS, C)[m, :, p, i - 1]
        if p:
            x = jnp.where(where == spot, south[m, i].reshape(1, LEVELS, C), x)
        return x.reshape(HALF * LEVELS, C).astype(F32)

    def norm(js, m):
        keys = [(j, q, p) for j in js for q in range(2) for p in range(2)]
        cells = {key: cell(m, *key) for key in keys}
        average, scale = {}, {}
        for j in js:
            total = sum(jnp.sum(cells[key], axis=1, keepdims=True) for key in keys if key[0] == j)
            average[j] = total * (1.0 / (4 * C))
        cells = {key: x - average[key[0]] for key, x in cells.items()}
        for j in js:
            total = sum(jnp.sum(cells[key] * cells[key], axis=1, keepdims=True) for key in keys if key[0] == j)
            scale[j] = lax.rsqrt(total * (1.0 / (4 * C)) + 1e-05)
        for j in js:
            done = []
            for q in range(2):
                for p in range(2):
                    g = 2 * q + p
                    y = cells[j, q, p] * scale[j] * gains[:, C * g : C * (g + 1)] + shifts[:, C * g : C * (g + 1)]
                    done.append(y.astype(BF))
            normed[j, m] = jnp.concatenate(done, axis=1)

    def inside():
        @pl.when(lat < 7)
        def _():
            for cp in to_prev:
                cp.wait_recv()

        @pl.when(lat > 0)
        def _():
            for cp in to_next:
                cp.wait_recv()
            tok[:, 0] = north[:, 1 : COLS + 1]

        for m in range(MEMBERS):
            norm((1, 2), m)

    def border(m):
        for cp in cols[m]:
            cp.wait_recv()
        norm((0, COLS // 2), m)

    def centre(w):
        blocks = [w[:, :C], w[:, C:]]
        return jnp.concatenate([v - jnp.sum(v, axis=1, keepdims=True) * (1.0 / C) for v in blocks], axis=1)

    def gather(home, finish, parts, keep, got, flat, rows, full, mine):
        count = 24 // rows

        @pl.when(home)
        def _():
            keep()

        for i in range(count):
            @pl.when(jnp.logical_not(jnp.logical_and(home, lat % count == i)))
            def _():
                copy(parts, got.at[i], s1_send.at[0], s1_recv.at[i], mate).wait_recv()

        for i in range(count):
            flat[rows * i : rows * (i + 1), :] = got[i].astype(F32)
        mine(z)[...] = finish(flat[...]).astype(BF).reshape(1, 24, 384)
        z_out = [copy(mine(z), mine(z), z_send.at[d], z_recv.at[d], along(d)) for d in ORDER]
        for cp in z_out:
            cp.start()
        for far in range(2):
            if COLS_AT[far] == -1:
                start_cols(far)
        started = []

        def pass_on(b, t):
            part = mine(b)
            for s in range(2):
                cp = copy(part, part, x_send.at[s, t], x_recv.at[s, t], across(1 + 2 * s))
                cp.start()
                started.append(cp)
            side = b % 2
            cp = copy(part, part, x_send.at[2, t], x_recv.at[2, t], (lon + side * (lon_o - lon), lat, mem_o) if MIX else across(2))
            cp.start()
            started.append(cp)

        def hand_over(b, t):
            for m in range(MEMBERS):
                if t == BORDER_AT[m]:
                    border(m)
            part = mine(b)
            for s in range(3):
                copy(part, part, x_send.at[s, t], x_recv.at[s, t], mate).wait_recv()
            whole = full.at[b]
            cp = copy(whole, whole, pair_send.at[t], pair_recv.at[t], mate)
            cp.start()
            started.append(cp)

        blocks = [(z + NZ - d) % NZ for d in (0,) + ARRIVE]
        for t, d in enumerate((0,) + ARRIVE):
            if d:
                copy(mine(z), mine(z), z_send.at[d], z_recv.at[d], mate).wait_recv()
            pass_on(blocks[t], t)
            for far in range(2):
                if COLS_AT[far] == t:
                    start_cols(far)
            if t == INSIDE:
                inside()
            if t >= LAG:
                hand_over(blocks[t - LAG], t - LAG)
        for t in range(NZ - LAG, NZ):
            hand_over(blocks[t], t)
        for m in range(MEMBERS):
            if BORDER_AT[m] == NZ:
                border(m)
        return z_out + started

    def take(other):
        for t, d in enumerate((0,) + ARRIVE):
            whole = other.at[(z + NZ - d) % NZ]
            copy(whole, whole, pair_send.at[t], pair_recv.at[t], mate).wait_recv()

    @pl.when(core == 0)
    def _():
        def keep():
            got_d[pl.ds(lat % 4, 1)] = own_d[...].reshape(1, 6, 384)

        def mine(b, n=1):
            return wd.at[pl.ds(b, n), pl.ds(pl.multiple_of(48 * cy + 24 * ch, 8), 24)]

        sent = gather(jnp.logical_and(yh == cy, lat // 4 == ch), lambda w: w, own_d, keep, got_d, flat, 6, wd, mine)
        take(wu)
        for cp in sent:
            cp.wait_send()

    @pl.when(core == 1)
    def _():
        def keep():
            got_u[pl.ds(lat, 1)] = own_u[:, pl.ds(pl.multiple_of(384 * ch, 128), 384)].reshape(1, 3, 384)

        def mine(b, n=1):
            return wu.at[pl.ds(b, n), pl.ds(pl.multiple_of(24 * cy, 8), 24), pl.ds(pl.multiple_of(384 * ch, 128), 384)]

        sent = gather(yh == cy, centre, own_u.at[:, :384], keep, got_u, flat, 3, wu, mine)
        take(wd)
        for cp in sent:
            cp.wait_send()

    each(lambda cp: cp.wait_send())
    for cp in cols[0] + cols[1]:
        cp.wait_send()

    @pl.when(lat < 7)
    def _():
        for cp in to_next:
            cp.wait_send()

    @pl.when(lat > 0)
    def _():
        for cp in to_prev:
            cp.wait_send()


def run_exchange(band_rows, tok, down, up, dg, ds):
    dma = pltpu.SemaphoreType.DMA
    vmem = pl.BlockSpec(memory_space=pltpu.VMEM)
    hbm = pl.BlockSpec(memory_space=pltpu.HBM)
    col = (MEMBERS, HALF, 3, LEVELS, 128)
    row = (MEMBERS, COLS + 2, LEVELS, C)
    return pl.pallas_call(
        exchange,
        out_shape=[
            jax.ShapeDtypeStruct((NZ, 96, 384), BF),
            jax.ShapeDtypeStruct((NZ, 48, 768), BF),
            jax.ShapeDtypeStruct((4, MEMBERS, HALF * LEVELS, 4 * C), BF),
        ],
        in_specs=[hbm] * 6,
        out_specs=[vmem] * 3,
        scratch_shapes=[
            pltpu.SMEM((1, 2), jnp.int32),
            pltpu.VMEM((4 * C,), F32),
            pltpu.VMEM((4 * C,), F32),
            pltpu.VMEM((MEMBERS, EXT, COLS, LEVELS, C), BF),
            pltpu.VMEM(col, BF),
            pltpu.VMEM(col, BF),
            pltpu.VMEM(col, BF),
            pltpu.VMEM(col, BF),
            pltpu.VMEM(row, BF),
            pltpu.VMEM(row, BF),
            pltpu.VMEM((MEMBERS, COLS, LEVELS, C), BF),
            pltpu.VMEM((6, 384), BF),
            pltpu.VMEM((3, 768), BF),
            pltpu.VMEM((4, 6, 384), BF),
            pltpu.VMEM((8, 3, 384), BF),
            pltpu.VMEM((24, 384), F32),
            dma((6,)), dma((8,)), dma((8,)), dma((NZ,)), dma((NZ,)), dma((3, NZ)), dma((3, NZ)),
            dma((NZ,)), dma((NZ,)), dma((2, 2)), dma((2, 2)), dma((6,)), dma((6,)),
        ],
        compiler_params=pltpu.CompilerParams(
            collective_id=0, has_side_effects=True, vmem_limit_bytes=24 << 20
        ),
        name="exchange",
    )(*(pltpu.with_memory_space_constraint(v, pltpu.HBM) for v in (band_rows, tok, down, up, dg, ds)))


SPLIT = ((0, 1),)
WIDE = 3
DEPTH = 1
ROWS = HALF * LEVELS


def patches(
    band_hbm, wd, wu, normed, ug, us, mix_hbm,
    out_hbm, band_ref, mix, fine, wu4, load_sem, store_sem,
):
    lat = lax.axis_index("lat")
    shift = jnp.minimum(lat, 1)
    loads = [
        pltpu.make_async_copy(mix_hbm, mix, load_sem.at[0]),
        pltpu.make_async_copy(band_hbm, band_ref, load_sem.at[1]),
    ]
    for load in loads:
        load.start()
    for g in range(4):
        wu4[g] = wu[:, C * g : C * (g + 1)]
    eps = 1e-05
    fine_gain, fine_shift = ug[...].reshape(1, C), us[...].reshape(1, C)
    pairs = out_hbm.reshape(MEMBERS, SLOTS // 2, 2, COLS, LEVELS, C)
    stores = []
    for members in SPLIT:
        def pick():
            return jnp.concatenate([normed[j, m] for j in range(4) for m in members], axis=0)

        coarse = jnp.dot(pick(), wd[...], preferred_element_type=F32).astype(BF)
        if members == SPLIT[0]:
            for load in loads:
                load.wait()
            bound = band_ref[0, 1] - band_ref[0, 0] + shift
        n = ROWS * len(members)
        keeps = [2 * lax.broadcasted_iota(jnp.int32, (HALF, LEVELS, C), 0) + p < bound for p in range(2)]

        def expand(p, q, j, w):
            r = n * (j + 1 - q)
            return jnp.dot(coarse[r : r + n * w], wu4[2 * p + q], preferred_element_type=F32)

        def settle(grown, p, q, j, w):
            spread = jnp.sum(grown * grown, axis=1, keepdims=True) * (1.0 / C)
            unit = (grown * lax.rsqrt(spread + eps) * fine_gain + fine_shift).astype(BF)
            done = jnp.dot(unit, mix[...], preferred_element_type=F32).astype(BF)
            done = done.reshape(w, len(members), HALF, LEVELS, C)
            for k in range(w):
                for i, m in enumerate(members):
                    fine[m, :, p, 2 * (j + k) + 1 - q] = jnp.where(keeps[p], done[k, i], jnp.zeros_like(done[k, i]))

        def leave(p):
            for m in members:
                store = pltpu.make_async_copy(
                    fine.at[m, pl.ds(shift * (1 - p), SLOTS // 2), p],
                    pairs.at[m, :, p + shift - 2 * p * shift],
                    store_sem.at[m, p],
                )
                store.start()
                stores.append(store)

        items = [(p, q, j, WIDE) for p in range(2) for q in range(2) for j in range(0, 3, WIDE)]
        ahead = []
        for item in items + [None] * DEPTH:
            if item is not None:
                ahead.append((item, expand(*item)))
            if len(ahead) > DEPTH or item is None:
                old, grown = ahead.pop(0)
                settle(grown, *old)
                if old[1] == 1 and old[2] + WIDE == 3:
                    leave(old[0])
    for store in stores:
        store.wait()


def run_patches(band_rows, wd, wu, normed, ug, us, mix):
    vmem = pl.BlockSpec(memory_space=pltpu.VMEM)
    hbm = pl.BlockSpec(memory_space=pltpu.HBM)
    band_rows, mix = (pltpu.with_memory_space_constraint(v, pltpu.HBM) for v in (band_rows, mix))
    return pl.pallas_call(
        patches,
        out_shape=jax.ShapeDtypeStruct((MEMBERS, SLOTS, COLS, LEVELS, C), BF),
        in_specs=[hbm] + [vmem] * 5 + [hbm],
        out_specs=pl.BlockSpec(memory_space=pl.ANY),
        scratch_shapes=[
            pltpu.SMEM((1, 2), jnp.int32),
            pltpu.VMEM((C, C), BF),
            pltpu.VMEM((MEMBERS, HALF, 2, COLS, LEVELS, C), BF),
            pltpu.VMEM((4, 2 * C, C), BF),
            pltpu.SemaphoreType.DMA((2,)),
            pltpu.SemaphoreType.DMA((MEMBERS, 2)),
        ],
        compiler_params=pltpu.CompilerParams(vmem_limit_bytes=24 << 20),
        name="patches",
    )(band_rows, wd, wu, normed, ug, us, mix)


def body(
    tokens, band_rows, down_gain, down_shift, down_weight, up_weight, up_gain, up_shift, mix_weight
):
    tok = tokens.transpose(0, 2, 3, 1, 4)
    wd, wu, normed = run_exchange(band_rows, tok, down_weight, up_weight, down_gain, down_shift)
    out = run_patches(
        band_rows, wd.reshape(4 * C, 2 * C), wu.reshape(2 * C, 4 * C), normed, up_gain, up_shift, mix_weight
    )
    return out.transpose(0, 3, 1, 2, 4)


def solution(mesh):
    return jax.shard_map(
        body,
        mesh=mesh,
        in_specs=(
            P("mem", None, "lat", "lon", None),
            P("lat", None),
            P(),
            P(),
            P(("lon", "lat"), None),
            P(("lon", "lat"), None),
            P(),
            P(),
            P(),
        ),
        out_specs=P("mem", None, "lat", "lon", None),
        check_vma=False,
    )
```

```python
import functools

import jax
import jax.numpy as jnp
from jax import lax
from jax.experimental import pallas as pl
from jax.experimental.pallas import tpu as pltpu
from jax.sharding import PartitionSpec as P

MESH = pl.DeviceIdType.MESH
MEMBERS, LEVELS, SLOTS, COLS, C = 2, 8, 34, 6, 192
EXT = SLOTS + 2
HALF = EXT // 2
NZ = 8
ORDER = (1, 7, 2, 6, 3, 5, 4)
ARRIVE = (1, 7, 2, 6, 3, 5, 4)
LAG = 6
BORDER_AT = (7, 8)
INSIDE = 0
COLS_AT = (-1, -1)
MIX = 0
BF = jnp.bfloat16
F32 = jnp.float32


def exchange(
    band_hbm, tok_hbm, down_hbm, up_hbm, dg_hbm, ds_hbm,
    wd, wu, normed,
    band_ref, dg, ds, tok, first_col, last_col, west, east, north, south, last, own_d, own_u, got_d, got_u, flat,
    load_sem, s1_send, s1_recv, z_send, z_recv, x_send, x_recv, pair_send, pair_recv,
    col_send, col_recv, row_send, row_recv,
):
    lon, lat, mem = lax.axis_index("lon"), lax.axis_index("lat"), lax.axis_index("mem")
    z, yh = lon // 2, lon % 2
    core, xx = lat % 2, lat // 2
    quarter = (xx + 2 * mem * MIX) % 4
    cy, ch = quarter % 2, quarter // 2
    shift = jnp.minimum(lat, 1)

    loads = [
        pltpu.make_async_copy(down_hbm, own_d, load_sem.at[0]),
        pltpu.make_async_copy(up_hbm, own_u, load_sem.at[1]),
        pltpu.make_async_copy(tok_hbm, tok.at[:, pl.ds(shift, SLOTS)], load_sem.at[2]),
        pltpu.make_async_copy(band_hbm, band_ref, load_sem.at[3]),
        pltpu.make_async_copy(dg_hbm, dg, load_sem.at[4]),
        pltpu.make_async_copy(ds_hbm, ds, load_sem.at[5]),
    ]
    for load in loads:
        load.start()

    @pl.when(lat > 0)
    def _():
        tok[:, 0] = jnp.zeros((MEMBERS, COLS, LEVELS, C), BF)
        tok[:, EXT - 1] = jnp.zeros((MEMBERS, COLS, LEVELS, C), BF)

    @pl.when(lat == 0)
    def _():
        tok[:, SLOTS:] = jnp.zeros((MEMBERS, 2, COLS, LEVELS, C), BF)

    lon_w, lon_e = (lon + 15) % 16, (lon + 1) % 16
    lat_n, lat_s = (lat + 7) % 8, (lat + 1) % 8
    lon_o, mem_o = 2 * z + 1 - yh, 1 - mem
    mate = (lon, lat + 1 - 2 * core, mem)

    def along(d):
        return (2 * ((z + d) % NZ) + yh, lat, mem)

    def across(s):
        return (lon, (lat + 2 * s) % 8, mem)

    barrier = pltpu.get_barrier_semaphore()
    partners = [(lon, (lat + d) % 8, mem) for d in range(1, 8)]
    partners += [(lon_o, (lat + d) % 8, mem_o) for d in range(8)]
    partners += [along(d) for d in range(1, NZ)]
    partners += [(lon, lat, mem_o)]
    partners += [
        (lon_w, lat, mem), (lon_e, lat, mem),
        (lon_w, lat_n, mem), (lon_w, lat_s, mem), (lon_e, lat_n, mem), (lon_e, lat_s, mem),
    ]
    for where in partners:
        pl.semaphore_signal(barrier, inc=1, device_id=where, device_id_type=MESH)
    loads[0].wait()
    loads[1].wait()
    pl.semaphore_wait(barrier, len(partners))

    def copy(src, dst, ssem, rsem, where):
        return pltpu.make_async_remote_copy(
            src_ref=src, dst_ref=dst, send_sem=ssem, recv_sem=rsem,
            device_id=where, device_id_type=MESH,
        )

    firsts = []

    def first(src, dst, i, slot, k, kind):
        lat_t = 2 * ((k + 2 * mem * MIX) % 4) + kind
        lat_f = 2 * ((k + 2 * mem_o * MIX) % 4) + kind
        firsts.append((lat_t != lat, copy(src, dst, s1_send.at[i], s1_recv.at[slot], (lon, lat_t, mem))))
        firsts.append((None, copy(src, dst, s1_send.at[i + 1], s1_recv.at[slot], (lon_o, lat_f, mem_o))))

    first(own_d, got_d.at[lat % 4], 0, lat % 4, yh + 2 * (lat // 4), 0)
    for h in range(2):
        first(own_u.at[:, 384 * h : 384 * (h + 1)], got_u.at[lat], 2 + 2 * h, lat, yh + 2 * h, 1)

    def each(op):
        for when, cp in firsts:
            if when is None:
                op(cp)
            else:
                @pl.when(when)
                def _():
                    op(cp)

    each(lambda cp: cp.start())

    for load in loads[2:]:
        load.wait()
    live = band_ref[0, 1] - band_ref[0, 0]
    last[...] = tok[:, pl.ds(jnp.clip(live - 1, 0, SLOTS - 1) + shift, 1)].reshape(MEMBERS, COLS, LEVELS, C)
    halves = tok.reshape(MEMBERS, HALF, 2, COLS, LEVELS, C)
    for m in range(MEMBERS):
        for i, box in ((0, first_col), (COLS - 1, last_col)):
            a, b = halves[m, :, 0, i], halves[m, :, 1, i]
            box[m, :, 0] = a[:, :, :128]
            box[m, :, 1] = b[:, :, :128]
            box[m, :, 2] = jnp.concatenate([a[:, :, 128:], b[:, :, 128:]], axis=2)

    cols = [
        [
            copy(first_col.at[m], east.at[m], col_send.at[m, 0], col_recv.at[m, 0], (lon_w, lat, mem)),
            copy(last_col.at[m], west.at[m], col_send.at[m, 1], col_recv.at[m, 1], (lon_e, lat, mem)),
        ]
        for m in range(MEMBERS)
    ]
    def start_cols(far):
        for m in range(MEMBERS):
            @pl.when(yh == far)
            def _():
                cols[m][1].start()

            @pl.when(yh != far)
            def _():
                cols[m][0].start()

    for far in range(2):
        if COLS_AT[far] == -2:
            start_cols(far)

    to_next = [
        copy(last, north.at[:, 1 : COLS + 1], row_send.at[0], row_recv.at[0], (lon, lat_s, mem)),
        copy(last.at[:, 0], north.at[:, COLS + 1], row_send.at[1], row_recv.at[1], (lon_w, lat_s, mem)),
        copy(last.at[:, COLS - 1], north.at[:, 0], row_send.at[2], row_recv.at[2], (lon_e, lat_s, mem)),
    ]
    to_prev = [
        copy(tok.at[:, shift], south.at[:, 1 : COLS + 1], row_send.at[3], row_recv.at[3], (lon, lat_n, mem)),
        copy(tok.at[:, shift, 0], south.at[:, COLS + 1], row_send.at[4], row_recv.at[4], (lon_w, lat_n, mem)),
        copy(tok.at[:, shift, COLS - 1], south.at[:, 0], row_send.at[5], row_recv.at[5], (lon_e, lat_n, mem)),
    ]

    @pl.when(lat < 7)
    def _():
        for cp in to_next:
            cp.start()

    @pl.when(lat > 0)
    def _():
        for cp in to_prev:
            cp.start()

    @pl.when(lat == 7)
    def _():
        south[...] = jnp.zeros_like(south)

    @pl.when(lat == 0)
    def _():
        north[...] = jnp.zeros_like(north)

    spot = (live + shift) // 2
    gains, shifts = dg[...].reshape(1, 4 * C), ds[...].reshape(1, 4 * C)

    def cell(m, j, q, p):
        i = 2 * j + q
        where = lax.broadcasted_iota(jnp.int32, (HALF, LEVELS, C), 0)
        if i in (0, COLS + 1):
            box = east if i else west
            x = jnp.concatenate([box[m, :, p], box[m, :, 2][:, :, 64 * p : 64 * p + 64]], axis=2)
            if p == 0:
                x = jnp.where(where + 1 == shift, north[m, i].reshape(1, LEVELS, C), x)
        else:
            x = tok.reshape(MEMBERS, HALF, 2, COLS, LEVELS, C)[m, :, p, i - 1]
        if p:
            x = jnp.where(where == spot, south[m, i].reshape(1, LEVELS, C), x)
        return x.reshape(HALF * LEVELS, C).astype(F32)

    def norm(js, m):
        keys = [(j, q, p) for j in js for q in range(2) for p in range(2)]
        cells = {key: cell(m, *key) for key in keys}
        average, scale = {}, {}
        for j in js:
            total = sum(jnp.sum(cells[key], axis=1, keepdims=True) for key in keys if key[0] == j)
            average[j] = total * (1.0 / (4 * C))
        cells = {key: x - average[key[0]] for key, x in cells.items()}
        for j in js:
            total = sum(jnp.sum(cells[key] * cells[key], axis=1, keepdims=True) for key in keys if key[0] == j)
            scale[j] = lax.rsqrt(total * (1.0 / (4 * C)) + 1e-05)
        for j in js:
            done = []
            for q in range(2):
                for p in range(2):
                    g = 2 * q + p
                    y = cells[j, q, p] * scale[j] * gains[:, C * g : C * (g + 1)] + shifts[:, C * g : C * (g + 1)]
                    done.append(y.astype(BF))
            normed[j, m] = jnp.concatenate(done, axis=1)

    def inside():
        @pl.when(lat < 7)
        def _():
            for cp in to_prev:
                cp.wait_recv()

        @pl.when(lat > 0)
        def _():
            for cp in to_next:
                cp.wait_recv()
            tok[:, 0] = north[:, 1 : COLS + 1]

        for m in range(MEMBERS):
            norm((1, 2), m)

    def border(m):
        for cp in cols[m]:
            cp.wait_recv()
        norm((0, COLS // 2), m)

    def centre(w):
        blocks = [w[:, :C], w[:, C:]]
        return jnp.concatenate([v - jnp.sum(v, axis=1, keepdims=True) * (1.0 / C) for v in blocks], axis=1)

    def gather(home, finish, parts, keep, got, flat, rows, full, mine):
        count = 24 // rows

        @pl.when(home)
        def _():
            keep()

        for i in range(count):
            @pl.when(jnp.logical_not(jnp.logical_and(home, lat % count == i)))
            def _():
                copy(parts, got.at[i], s1_send.at[0], s1_recv.at[i], mate).wait_recv()

        for i in range(count):
            flat[rows * i : rows * (i + 1), :] = got[i].astype(F32)
        mine(z)[...] = finish(flat[...]).astype(BF).reshape(1, 24, 384)
        z_out = [copy(mine(z), mine(z), z_send.at[d], z_recv.at[d], along(d)) for d in ORDER]
        for cp in z_out:
            cp.start()
        for far in range(2):
            if COLS_AT[far] == -1:
                start_cols(far)
        started = []

        def pass_on(b, t):
            part = mine(b)
            for s in range(2):
                cp = copy(part, part, x_send.at[s, t], x_recv.at[s, t], across(1 + 2 * s))
                cp.start()
                started.append(cp)
            side = b % 2
            cp = copy(part, part, x_send.at[2, t], x_recv.at[2, t], (lon + side * (lon_o - lon), lat, mem_o) if MIX else across(2))
            cp.start()
            started.append(cp)

        def hand_over(b, t):
            for m in range(MEMBERS):
                if t == BORDER_AT[m]:
                    border(m)
            part = mine(b)
            for s in range(3):
                copy(part, part, x_send.at[s, t], x_recv.at[s, t], mate).wait_recv()
            whole = full.at[b]
            cp = copy(whole, whole, pair_send.at[t], pair_recv.at[t], mate)
            cp.start()
            started.append(cp)

        blocks = [(z + NZ - d) % NZ for d in (0,) + ARRIVE]
        for t, d in enumerate((0,) + ARRIVE):
            if d:
                copy(mine(z), mine(z), z_send.at[d], z_recv.at[d], mate).wait_recv()
            pass_on(blocks[t], t)
            for far in range(2):
                if COLS_AT[far] == t:
                    start_cols(far)
            if t == INSIDE:
                inside()
            if t >= LAG:
                hand_over(blocks[t - LAG], t - LAG)
        for t in range(NZ - LAG, NZ):
            hand_over(blocks[t], t)
        for m in range(MEMBERS):
            if BORDER_AT[m] == NZ:
                border(m)
        return z_out + started

    def take(other):
        for t, d in enumerate((0,) + ARRIVE):
            whole = other.at[(z + NZ - d) % NZ]
            copy(whole, whole, pair_send.at[t], pair_recv.at[t], mate).wait_recv()

    @pl.when(core == 0)
    def _():
        def keep():
            got_d[pl.ds(lat % 4, 1)] = own_d[...].reshape(1, 6, 384)

        def mine(b, n=1):
            return wd.at[pl.ds(b, n), pl.ds(pl.multiple_of(48 * cy + 24 * ch, 8), 24)]

        sent = gather(jnp.logical_and(yh == cy, lat // 4 == ch), lambda w: w, own_d, keep, got_d, flat, 6, wd, mine)
        take(wu)
        for cp in sent:
            cp.wait_send()

    @pl.when(core == 1)
    def _():
        def keep():
            got_u[pl.ds(lat, 1)] = own_u[:, pl.ds(pl.multiple_of(384 * ch, 128), 384)].reshape(1, 3, 384)

        def mine(b, n=1):
            return wu.at[pl.ds(b, n), pl.ds(pl.multiple_of(24 * cy, 8), 24), pl.ds(pl.multiple_of(384 * ch, 128), 384)]

        sent = gather(yh == cy, centre, own_u.at[:, :384], keep, got_u, flat, 3, wu, mine)
        take(wd)
        for cp in sent:
            cp.wait_send()

    each(lambda cp: cp.wait_send())
    for cp in cols[0] + cols[1]:
        cp.wait_send()

    @pl.when(lat < 7)
    def _():
        for cp in to_next:
            cp.wait_send()

    @pl.when(lat > 0)
    def _():
        for cp in to_prev:
            cp.wait_send()


def run_exchange(band_rows, tok, down, up, dg, ds):
    dma = pltpu.SemaphoreType.DMA
    vmem = pl.BlockSpec(memory_space=pltpu.VMEM)
    hbm = pl.BlockSpec(memory_space=pltpu.HBM)
    col = (MEMBERS, HALF, 3, LEVELS, 128)
    row = (MEMBERS, COLS + 2, LEVELS, C)
    return pl.pallas_call(
        exchange,
        out_shape=[
            jax.ShapeDtypeStruct((NZ, 96, 384), BF),
            jax.ShapeDtypeStruct((NZ, 48, 768), BF),
            jax.ShapeDtypeStruct((4, MEMBERS, HALF * LEVELS, 4 * C), BF),
        ],
        in_specs=[hbm] * 6,
        out_specs=[vmem] * 3,
        scratch_shapes=[
            pltpu.SMEM((1, 2), jnp.int32),
            pltpu.VMEM((4 * C,), F32),
            pltpu.VMEM((4 * C,), F32),
            pltpu.VMEM((MEMBERS, EXT, COLS, LEVELS, C), BF),
            pltpu.VMEM(col, BF),
            pltpu.VMEM(col, BF),
            pltpu.VMEM(col, BF),
            pltpu.VMEM(col, BF),
            pltpu.VMEM(row, BF),
            pltpu.VMEM(row, BF),
            pltpu.VMEM((MEMBERS, COLS, LEVELS, C), BF),
            pltpu.VMEM((6, 384), BF),
            pltpu.VMEM((3, 768), BF),
            pltpu.VMEM((4, 6, 384), BF),
            pltpu.VMEM((8, 3, 384), BF),
            pltpu.VMEM((24, 384), F32),
            dma((6,)), dma((8,)), dma((8,)), dma((NZ,)), dma((NZ,)), dma((3, NZ)), dma((3, NZ)),
            dma((NZ,)), dma((NZ,)), dma((2, 2)), dma((2, 2)), dma((6,)), dma((6,)),
        ],
        compiler_params=pltpu.CompilerParams(
            collective_id=0, has_side_effects=True, vmem_limit_bytes=24 << 20
        ),
        name="exchange",
    )(*(pltpu.with_memory_space_constraint(v, pltpu.HBM) for v in (band_rows, tok, down, up, dg, ds)))


SPLIT = ((0, 1),)
WIDE = 3
DEPTH = 1
ROWS = HALF * LEVELS


def patches(
    band_hbm, wd, wu, normed, ug, us, mix_hbm,
    out_hbm, band_ref, mix, fine, load_sem, store_sem,
):
    lat = lax.axis_index("lat")
    shift = jnp.minimum(lat, 1)
    loads = [
        pltpu.make_async_copy(mix_hbm, mix, load_sem.at[0]),
        pltpu.make_async_copy(band_hbm, band_ref, load_sem.at[1]),
    ]
    for load in loads:
        load.start()
    eps = 1e-05
    fine_gain, fine_shift = ug[...].reshape(1, C), us[...].reshape(1, C)
    pairs = out_hbm.reshape(MEMBERS, SLOTS // 2, 2, COLS, LEVELS, C)
    stores = []
    for members in SPLIT:
        def pick():
            return jnp.concatenate([normed[j, m] for j in range(4) for m in members], axis=0)

        coarse = jnp.dot(pick(), wd[...], preferred_element_type=F32).astype(BF)
        if members == SPLIT[0]:
            for load in loads:
                load.wait()
            bound = band_ref[0, 1] - band_ref[0, 0] + shift
        n = ROWS * len(members)
        keeps = [2 * lax.broadcasted_iota(jnp.int32, (HALF, LEVELS, C), 0) + p < bound for p in range(2)]

        def expand(p, q, j, w):
            r = n * (j + 1 - q)
            return jnp.dot(coarse[r : r + n * w], wu[:, C * (2 * p + q) : C * (2 * p + q + 1)], preferred_element_type=F32)

        def settle(grown, p, q, j, w):
            spread = jnp.sum(grown * grown, axis=1, keepdims=True) * (1.0 / C)
            unit = (grown * lax.rsqrt(spread + eps) * fine_gain + fine_shift).astype(BF)
            done = jnp.dot(unit, mix[...], preferred_element_type=F32).astype(BF)
            done = done.reshape(w, len(members), HALF, LEVELS, C)
            for k in range(w):
                for i, m in enumerate(members):
                    fine[m, :, p, 2 * (j + k) + 1 - q] = jnp.where(keeps[p], done[k, i], jnp.zeros_like(done[k, i]))

        def leave(p):
            for m in members:
                store = pltpu.make_async_copy(
                    fine.at[m, pl.ds(shift * (1 - p), SLOTS // 2), p],
                    pairs.at[m, :, p + shift - 2 * p * shift],
                    store_sem.at[m, p],
                )
                store.start()
                stores.append(store)

        items = [(p, q, j, WIDE) for p in range(2) for q in range(2) for j in range(0, 3, WIDE)]
        ahead = []
        for item in items + [None] * DEPTH:
            if item is not None:
                ahead.append((item, expand(*item)))
            if len(ahead) > DEPTH or item is None:
                old, grown = ahead.pop(0)
                settle(grown, *old)
                if old[1] == 1 and old[2] + WIDE == 3:
                    leave(old[0])
    for store in stores:
        store.wait()


def run_patches(band_rows, wd, wu, normed, ug, us, mix):
    vmem = pl.BlockSpec(memory_space=pltpu.VMEM)
    hbm = pl.BlockSpec(memory_space=pltpu.HBM)
    band_rows, mix = (pltpu.with_memory_space_constraint(v, pltpu.HBM) for v in (band_rows, mix))
    return pl.pallas_call(
        patches,
        out_shape=jax.ShapeDtypeStruct((MEMBERS, SLOTS, COLS, LEVELS, C), BF),
        in_specs=[hbm] + [vmem] * 5 + [hbm],
        out_specs=pl.BlockSpec(memory_space=pl.ANY),
        scratch_shapes=[
            pltpu.SMEM((1, 2), jnp.int32),
            pltpu.VMEM((C, C), BF),
            pltpu.VMEM((MEMBERS, HALF, 2, COLS, LEVELS, C), BF),
            pltpu.SemaphoreType.DMA((2,)),
            pltpu.SemaphoreType.DMA((MEMBERS, 2)),
        ],
        compiler_params=pltpu.CompilerParams(vmem_limit_bytes=24 << 20),
        name="patches",
    )(band_rows, wd, wu, normed, ug, us, mix)


def body(
    tokens, band_rows, down_gain, down_shift, down_weight, up_weight, up_gain, up_shift, mix_weight
):
    tok = tokens.transpose(0, 2, 3, 1, 4)
    wd, wu, normed = run_exchange(band_rows, tok, down_weight, up_weight, down_gain, down_shift)
    out = run_patches(
        band_rows, wd.reshape(4 * C, 2 * C), wu.reshape(2 * C, 4 * C), normed, up_gain, up_shift, mix_weight
    )
    return out.transpose(0, 3, 1, 2, 4)


def solution(mesh):
    return jax.shard_map(
        body,
        mesh=mesh,
        in_specs=(
            P("mem", None, "lat", "lon", None),
            P("lat", None),
            P(),
            P(),
            P(("lon", "lat"), None),
            P(("lon", "lat"), None),
            P(),
            P(),
            P(),
        ),
        out_specs=P("mem", None, "lat", "lon", None),
        check_vma=False,
    )
```
